32 devices in a mesh: dp: 2 (over x), tp: 4 (over z), pp: 4 (over y, core).
Axes of the slice: x: 2, y: 2, z: 4, core: 2. Of those that a mesh axis runs over, the one named last changes fastest.
Arguments:
- x_in: bfloat16 [8, 1, 128, 2560], P('dp'), parts along dimension 0
- seq_lens: int32 [8, 1], P('dp'), parts along dimension 0
- ln1_gain: bfloat16 [4, 2560], P('pp')
- ln1_shift: bfloat16 [4, 2560], P('pp')
- w_qkv: bfloat16 [4, 2560, 3, 2560], P('pp', None, None, 'tp')
- b_qkv: bfloat16 [4, 3, 32, 80], P('pp', None, 'tp')
- w_out: bfloat16 [4, 2560, 2560], P('pp', 'tp')
- b_out: bfloat16 [4, 2560], P('pp')
- ln2_gain: bfloat16 [4, 2560], P('pp')
- ln2_shift: bfloat16 [4, 2560], P('pp')
- w_up: bfloat16 [4, 2560, 10240], P('pp', None, 'tp')
- b_up: bfloat16 [4, 10240], P('pp', 'tp')
- w_down: bfloat16 [4, 10240, 2560], P('pp', 'tp')
- b_down: bfloat16 [4, 2560], P('pp')
Outputs:
- output: bfloat16 [4, 8, 1, 128, 2560], P('pp', 'dp'), parts along dimension 1
There are 2 independent parts. The reference program is written for one: setup_inputs(seed, part) draws one part's arguments, and reference() takes and returns one part's arrays. A program takes and returns all parts, laid end to end along the dimension named above; an argument that names none is the same for every part.
All inputs are finite; a program needn't handle non-finite values.
Results may differ from the reference program's by a relative error of at most 0.0189996.
Values are sent between devices in bfloat16 or wider.
A program may use at most 1 GiB of HBM per device.

```python
import jax
import jax.numpy as jnp
from jax import lax
import math

LAYERS = 4
MICRO_COUNT = 4
BATCH_SIZE = 1
SEQ_LEN = 128
MODEL_DIM = 2560
NUM_HEADS = 32
HIDDEN_DIM = 10240
HEAD_DIM = MODEL_DIM // NUM_HEADS


def alibi_slopes(heads_n):
    closest = 2 ** int(math.floor(math.log2(heads_n)))
    base_rate = 2.0 ** (-8.0 / closest)
    slope_list = [base_rate ** (head_idx + 1) for head_idx in range(closest)]
    extra_rate = 2.0 ** (-4.0 / closest)
    slope_list = slope_list + [extra_rate ** (2 * head_idx + 1) for head_idx in range(min(closest, heads_n - closest))]
    return jnp.array(slope_list, dtype=jnp.float32)


def layer_norm(values, gain_vec, shift_vec):
    val_f = values.astype(jnp.float32)
    mean_val = jnp.mean(val_f, axis=-1, keepdims=True)
    centered = val_f - mean_val
    var_val = jnp.mean(centered * centered, axis=-1, keepdims=True)
    normed = centered * lax.rsqrt(var_val + 1e-5)
    return (normed * gain_vec.astype(jnp.float32) + shift_vec.astype(jnp.float32)).astype(jnp.bfloat16)


def attention(query_all, key_all, val_all, slopes, lens_row):
    batch_n, seq_n, heads_n, head_dim = query_all.shape
    blk_len = min(seq_n, 128)
    key_pos = jnp.arange(seq_n)
    key_ok = key_pos[None, :] < lens_row[:, None]
    key_f = key_all.astype(jnp.float32)
    val_f = val_all.astype(jnp.float32)

    def one_block(blk_idx):
        query_blk = lax.dynamic_slice_in_dim(query_all, blk_idx * blk_len, blk_len, 1).astype(jnp.float32)
        scores = jnp.einsum('bqhe,bkhe->bhqk', query_blk, key_f) * (head_dim ** -0.5)
        query_pos = blk_idx * blk_len + jnp.arange(blk_len)
        distance = (query_pos[:, None] - key_pos[None, :]).astype(jnp.float32)
        scores = scores - slopes[None, :, None, None] * distance[None, None]
        allowed = (key_pos[None, :] <= query_pos[:, None])[None, None] & key_ok[:, None, None, :]
        scores = jnp.where(allowed, scores, -1e30)
        prob_bf = jax.nn.softmax(scores, axis=-1).astype(jnp.bfloat16)
        return jnp.einsum('bhqk,bkhe->bqhe', prob_bf.astype(jnp.float32), val_f).astype(jnp.bfloat16)

    blocks = lax.map(one_block, jnp.arange(seq_n // blk_len))
    return jnp.moveaxis(blocks, 0, 1).reshape(batch_n, seq_n, heads_n * head_dim)


def bloom_layer(act_in, lens_row, layer_w, slopes):
    ln1_gain, ln1_shift, w_qkv, b_qkv, w_out, b_out, ln2_gain, ln2_shift, w_up, b_up, w_down, b_down = layer_w
    batch_n, seq_n, model_n = act_in.shape
    tokens_n = batch_n * seq_n
    heads_n, head_dim = b_qkv.shape[1], b_qkv.shape[2]
    flat_in = act_in.reshape(tokens_n, model_n)
    normed = layer_norm(flat_in, ln1_gain, ln1_shift)
    qkv_all = (jnp.dot(normed, w_qkv.reshape(model_n, 3 * model_n), preferred_element_type=jnp.float32) + b_qkv.reshape(3 * model_n).astype(jnp.float32)).astype(jnp.bfloat16)
    qkv_all = qkv_all.reshape(batch_n, seq_n, 3, heads_n, head_dim)
    context = attention(qkv_all[:, :, 0], qkv_all[:, :, 1], qkv_all[:, :, 2], slopes, lens_row)
    attn_out = jnp.dot(context.reshape(tokens_n, model_n), w_out, preferred_element_type=jnp.float32)
    resid_act = (flat_in.astype(jnp.float32) + attn_out + b_out.astype(jnp.float32)).astype(jnp.bfloat16)
    normed_mlp = layer_norm(resid_act, ln2_gain, ln2_shift)
    hidden_act = jax.nn.gelu(jnp.dot(normed_mlp, w_up, preferred_element_type=jnp.float32) + b_up.astype(jnp.float32), approximate=True).astype(jnp.bfloat16)
    mlp_out = jnp.dot(hidden_act, w_down, preferred_element_type=jnp.float32)
    result = (resid_act.astype(jnp.float32) + mlp_out + b_down.astype(jnp.float32)).astype(jnp.bfloat16)
    return result.reshape(batch_n, seq_n, model_n)


def setup_inputs(seed: int = 0, part: int = 0) -> dict:
    w_keys = jax.random.split(jax.random.key(seed), 12)
    part_keys = jax.random.split(jax.random.fold_in(jax.random.key(seed + 1), part), 2)

    def normal_draw(rng_key, arr_shape, std_dev, offset):
        return (offset + std_dev * jax.random.normal(rng_key, arr_shape, jnp.float32)).astype(jnp.bfloat16)

    width_scale = MODEL_DIM ** -0.5
    lens_draw = jax.random.randint(part_keys[1], (MICRO_COUNT, BATCH_SIZE), 1, SEQ_LEN + 1, dtype=jnp.int32)
    return dict(
        x_in=normal_draw(part_keys[0], (MICRO_COUNT, BATCH_SIZE, SEQ_LEN, MODEL_DIM), 1.0, 0.0),
        seq_lens=lens_draw.at[0, 0].set(SEQ_LEN),
        ln1_gain=normal_draw(w_keys[0], (LAYERS, MODEL_DIM), 0.3, 1.0),
        ln1_shift=normal_draw(w_keys[1], (LAYERS, MODEL_DIM), 0.3, 0.0),
        w_qkv=normal_draw(w_keys[2], (LAYERS, MODEL_DIM, 3, MODEL_DIM), width_scale, 0.0),
        b_qkv=normal_draw(w_keys[3], (LAYERS, 3, NUM_HEADS, HEAD_DIM), 0.3, 0.0),
        w_out=normal_draw(w_keys[4], (LAYERS, MODEL_DIM, MODEL_DIM), width_scale, 0.0),
        b_out=normal_draw(w_keys[5], (LAYERS, MODEL_DIM), 0.3, 0.0),
        ln2_gain=normal_draw(w_keys[6], (LAYERS, MODEL_DIM), 0.3, 1.0),
        ln2_shift=normal_draw(w_keys[7], (LAYERS, MODEL_DIM), 0.3, 0.0),
        w_up=normal_draw(w_keys[8], (LAYERS, MODEL_DIM, HIDDEN_DIM), width_scale, 0.0),
        b_up=normal_draw(w_keys[9], (LAYERS, HIDDEN_DIM), 0.3, 0.0),
        w_down=normal_draw(w_keys[10], (LAYERS, HIDDEN_DIM, MODEL_DIM), HIDDEN_DIM ** -0.5, 0.0),
        b_down=normal_draw(w_keys[11], (LAYERS, MODEL_DIM), 0.3, 0.0),
    )


def reference(x_in, seq_lens, ln1_gain, ln1_shift, w_qkv, b_qkv, w_out, b_out, ln2_gain, ln2_shift, w_up, b_up, w_down, b_down):
    slopes = alibi_slopes(NUM_HEADS)

    def layer_step(current, layer_w):
        new_act = lax.map(lambda micro_pair: bloom_layer(micro_pair[0], micro_pair[1], layer_w, slopes), (current, seq_lens))
        return new_act, new_act

    final_act, hidden = lax.scan(layer_step, x_in, (ln1_gain, ln1_shift, w_qkv, b_qkv, w_out, b_out, ln2_gain, ln2_shift, w_up, b_up, w_down, b_down))
    return hidden
```

```python
import functools
import math

import jax
import jax.numpy as jnp
from jax import lax
from jax.experimental import pallas as pl
from jax.experimental.pallas import tpu as pltpu
from jax.sharding import PartitionSpec as P

MESH = pl.DeviceIdType.MESH
CH = 512


def alibi_slopes(heads_n):
    closest = 2 ** int(math.floor(math.log2(heads_n)))
    base_rate = 2.0 ** (-8.0 / closest)
    slope_list = [base_rate ** (head_idx + 1) for head_idx in range(closest)]
    extra_rate = 2.0 ** (-4.0 / closest)
    slope_list = slope_list + [extra_rate ** (2 * head_idx + 1) for head_idx in range(min(closest, heads_n - closest))]
    return jnp.array(slope_list, dtype=jnp.float32)


def kernel(stages, micro_n, seq_n, model_n, hid_loc, heads_loc, head_dim,
           lens_ref, slopes_ref, x_hbm, wqkv_hbm, wout_hbm, wup_hbm, wdown_hbm,
           g1_ref, s1_ref, bqkv_ref, bo_ref, g2_ref, s2_ref, bup_ref, bd_ref,
           out_hbm,
           wqkv, wout, wup, wdown, xbuf, in1, in2, part, a_ref, u_ref, qkv, ctx, ctxb,
           wq_sem, wo_sem, wu_sem, wd_sem, x_sem, in1_sem, in2_sem, s1_sem, s2_sem, f_sem, o_sem):
    tp = lax.axis_index('tp')
    pp = lax.axis_index('pp')
    nc = model_n // CH
    nu = hid_loc // CH
    inner = (tp == 1) | (tp == 2)
    outer = (tp == 0) | (tp == 3)
    partner = tp + 1 - 2 * (tp % 2)
    peer = 3 - tp
    first = pp == 0
    later = pp > 0
    sends = pp < stages - 1

    def x_copy(u, c):
        return pltpu.make_async_copy(x_hbm.at[u, :, pl.ds(c * CH, CH)], xbuf.at[u, c], x_sem.at[u, c])

    def wq_copy(c):
        return pltpu.make_async_copy(wqkv_hbm.at[c], wqkv.at[c], wq_sem.at[c])

    def wo_copy(c):
        return pltpu.make_async_copy(wout_hbm.at[:, pl.ds(c * CH, CH)], wout.at[c], wo_sem.at[c])

    def wu_copy(c):
        return pltpu.make_async_copy(wup_hbm.at[:, pl.ds(c * CH, CH)], wup.at[c], wu_sem.at[c])

    def wd_copy(c):
        return pltpu.make_async_copy(wdown_hbm.at[:, pl.ds(c * CH, CH)], wdown.at[c], wd_sem.at[c])

    @pl.when(first)
    def _():
        for c in range(nc):
            x_copy(0, c).start()
    for c in range(3):
        wq_copy(c).start()
    for c in range(nc):
        wo_copy(c).start()
    for c in range(nu):
        wu_copy(c).start()
    for c in range(nc):
        wd_copy(c).start()

    @pl.when(first)
    def _():
        for u in range(1, micro_n):
            for c in range(nc):
                x_copy(u, c).start()

    barrier = pltpu.get_barrier_semaphore()
    links = ((tp > 0, {'tp': tp - 1}), (tp < 3, {'tp': tp + 1}), (later, {'pp': pp - 1}), (sends, {'pp': pp + 1}))
    for cond, dev in links:
        @pl.when(cond)
        def _(dev=dev):
            pl.semaphore_signal(barrier, inc=1, device_id=dev, device_id_type=MESH)
    pl.semaphore_wait(barrier, sum(cond.astype(jnp.int32) for cond, _ in links))

    def part_copy(k, c):
        return pltpu.make_async_remote_copy(
            src_ref=part.at[k % 2, c], dst_ref=in1.at[k, c], send_sem=s1_sem.at[k, c], recv_sem=in1_sem.at[k, c],
            device_id={'tp': partner}, device_id_type=MESH)

    def sum_copy(k, c):
        return pltpu.make_async_remote_copy(
            src_ref=part.at[k % 2, c], dst_ref=in2.at[k, c], send_sem=s1_sem.at[k, c], recv_sem=in2_sem.at[k, c],
            device_id={'tp': peer}, device_id_type=MESH)

    def res_copy(k, c):
        return pltpu.make_async_remote_copy(
            src_ref=in1.at[k, c], dst_ref=in1.at[k, c], send_sem=s2_sem.at[k, c], recv_sem=in1_sem.at[k, c],
            device_id={'tp': partner}, device_id_type=MESH)

    def fwd_copy(u, c):
        return pltpu.make_async_remote_copy(
            src_ref=in1.at[2 * u + 1, c], dst_ref=xbuf.at[u, c], send_sem=f_sem.at[u, c], recv_sem=x_sem.at[u, c],
            device_id={'pp': pp + 1}, device_id_type=MESH)

    def out_copy(u, c):
        return pltpu.make_async_copy(in1.at[2 * u + 1, c], out_hbm.at[u, :, pl.ds(c * CH, CH)], o_sem.at[u, c])

    def cols(c, width=CH):
        return pl.ds(pl.multiple_of(c * width, width), width)

    rows_blk = 32

    def layer_norm(src, idx, gain, shift):
        @pl.loop(0, seq_n // rows_blk)
        def _(r):
            rows = pl.ds(pl.multiple_of(r * rows_blk, rows_blk), rows_blk)
            val = jnp.concatenate([src[idx, c, rows, :] for c in range(nc)], axis=-1).astype(jnp.float32)
            mean = jnp.sum(val, axis=-1, keepdims=True) * (1.0 / model_n)
            cen = val - mean
            var = jnp.sum(cen * cen, axis=-1, keepdims=True) * (1.0 / model_n)
            normed = cen * lax.rsqrt(var + 1e-5)
            a_ref[rows, :] = (normed * gain[...].astype(jnp.float32) + shift[...].astype(jnp.float32)).astype(jnp.bfloat16)

    def attention(u):
        seq_len = lens_ref[u]
        qpos = lax.broadcasted_iota(jnp.int32, (seq_n, seq_n), 0)
        kpos = lax.broadcasted_iota(jnp.int32, (seq_n, seq_n), 1)
        allowed = (kpos <= qpos) & (kpos < seq_len)
        dist = (qpos - kpos).astype(jnp.float32)
        ctx[...] = jnp.zeros_like(ctx)

        @pl.loop(0, heads_loc // 2)
        def _(g):
            win = pl.ds(pl.multiple_of(g * 128, 128), 256)
            lane = lax.broadcasted_iota(jnp.int32, (1, 256), 1) + g * 128
            low = 2 * head_dim * g
            m0 = ((lane >= low) & (lane < low + head_dim)).astype(jnp.float32).astype(jnp.bfloat16)
            m1 = ((lane >= low + head_dim) & (lane < low + 2 * head_dim)).astype(jnp.float32).astype(jnp.bfloat16)
            key = qkv[1, :, win]
            val = qkv[2, :, win]
            kk = jnp.concatenate([key * m0, key * m1], axis=0)
            vv = jnp.concatenate([val * m0, val * m1], axis=0)
            sc = lax.dot_general(qkv[0, :, win], kk, (((1,), (1,)), ((), ())), preferred_element_type=jnp.float32)
            probs = []
            for j in range(2):
                s = sc[:, j * seq_n:(j + 1) * seq_n] * (head_dim ** -0.5)
                s = s - slopes_ref[tp * heads_loc + 2 * g + j] * dist
                s = jnp.where(allowed, s, -1e30)
                e = jnp.exp(s - jnp.max(s, axis=-1, keepdims=True))
                probs.append((e / jnp.sum(e, axis=-1, keepdims=True)).astype(jnp.bfloat16))
            o = jnp.dot(jnp.concatenate(probs, axis=-1), vv, preferred_element_type=jnp.float32)
            ctx[:, win] += o
        ctxb[...] = ctx[...].astype(jnp.bfloat16)

    def own_partial(s, a, lhs, w, w_copy):
        k = 2 * s + a

        @pl.loop(0, nc)
        def _(c):
            @pl.when(s == 0)
            def _():
                w_copy(c).wait()

            @pl.when(s > 0)
            def _():
                part_copy(k - 2, c).wait_send()
            part[a, c] = jnp.dot(lhs[...], w[c], preferred_element_type=jnp.float32).astype(jnp.bfloat16)

            @pl.when(outer)
            def _():
                part_copy(k, c).start()

    def p1(s):
        for c in range(nc):
            x_copy(s, c).wait()
        layer_norm(xbuf, s, g1_ref, s1_ref)

        for c in range(3):
            @pl.when(s == 0)
            def _(c=c):
                wq_copy(c).wait()
            acc = jnp.dot(a_ref[...], wqkv[c], preferred_element_type=jnp.float32)
            qkv[c] = (acc + bqkv_ref[c:c + 1, :].astype(jnp.float32)).astype(jnp.bfloat16)
        attention(s)
        own_partial(s, 0, ctxb, wout, wo_copy)

    def p2(s):
        layer_norm(in1, 2 * s, g2_ref, s2_ref)

        @pl.loop(0, nu)
        def _(c):
            @pl.when(s == 0)
            def _():
                wu_copy(c).wait()
            t = jnp.dot(a_ref[...], wup[c], preferred_element_type=jnp.float32) + bup_ref[:, cols(c)].astype(jnp.float32)
            t = 0.5 * t * (1.0 + jnp.tanh(math.sqrt(2.0 / math.pi) * (t + 0.044715 * (t * t * t))))
            u_ref[:, cols(c)] = t.astype(jnp.bfloat16)
        own_partial(s, 1, u_ref, wdown, wd_copy)

    def r1(s, a):
        k = 2 * s + a

        @pl.when(inner)
        def _():
            @pl.loop(0, nc)
            def _(c):
                part_copy(k, c).wait_recv()
                part[a, c] = (part[a, c].astype(jnp.float32) + in1[k, c].astype(jnp.float32)).astype(jnp.bfloat16)
                sum_copy(k, c).start()

    def r2(s, a):
        k = 2 * s + a
        bias = bo_ref if a == 0 else bd_ref

        @pl.loop(0, nc)
        def _(c):
            @pl.when(inner)
            def _():
                sum_copy(k, c).wait_recv()
                resid = xbuf[s, c] if a == 0 else in1[2 * s, c]
                total = part[a, c].astype(jnp.float32) + in2[k, c].astype(jnp.float32)
                in1[k, c] = (resid.astype(jnp.float32) + total + bias[:, cols(c)].astype(jnp.float32)).astype(jnp.bfloat16)
                res_copy(k, c).start()

            @pl.when(outer)
            def _():
                part_copy(k, c).wait_recv()
            if a == 1:
                @pl.when(sends)
                def _():
                    fwd_copy(s, c).start()
                out_copy(s, c).start()

    @pl.loop(0, micro_n + 1)
    def _(s):
        @pl.when(s > 0)
        def _():
            r1(s - 1, 1)

        @pl.when(s < micro_n)
        def _():
            p1(s)

        @pl.when(s > 0)
        def _():
            r2(s - 1, 1)

        @pl.when(s < micro_n)
        def _():
            r1(s, 0)
            r2(s, 0)
            p2(s)

    last = micro_n - 1
    for a in range(2):
        for c in range(nc):
            part_copy(2 * last + a, c).wait_send()

    @pl.when(inner)
    def _():
        @pl.loop(0, 2 * micro_n)
        def _(k):
            @pl.loop(0, nc)
            def _(c):
                res_copy(k, c).wait_send()

    @pl.loop(0, micro_n)
    def _(u):
        @pl.loop(0, nc)
        def _(c):
            @pl.when(sends)
            def _():
                fwd_copy(u, c).wait_send()
            out_copy(u, c).wait()


def solution(mesh):
    stages = mesh.shape['pp']
    in_specs = (P('dp'), P('dp'), P('pp'), P('pp'), P('pp', None, None, 'tp'), P('pp', None, 'tp', None), P('pp', 'tp', None), P('pp'), P('pp'), P('pp'), P('pp', None, 'tp'), P('pp', 'tp'), P('pp', 'tp', None), P('pp'))

    def per_device(x_in, seq_lens, ln1_gain, ln1_shift, w_qkv, b_qkv, w_out, b_out, ln2_gain, ln2_shift, w_up, b_up, w_down, b_down):
        micro_n, batch_n, seq_n, model_n = x_in.shape
        heads_loc, head_dim = b_qkv.shape[2], b_qkv.shape[3]
        width_loc = heads_loc * head_dim
        hid_loc = w_up.shape[2]
        nc, nu = model_n // CH, hid_loc // CH
        assert batch_n == 1 and mesh.shape['tp'] == 4 and seq_n == 128
        slopes = alibi_slopes(heads_loc * mesh.shape['tp'])
        bf = jnp.bfloat16
        vm = pl.BlockSpec(memory_space=pltpu.VMEM)
        sm = pl.BlockSpec(memory_space=pltpu.SMEM)
        hb = pl.BlockSpec(memory_space=pl.ANY)
        dma = pltpu.SemaphoreType.DMA
        body = functools.partial(kernel, stages, micro_n, seq_n, model_n, hid_loc, heads_loc, head_dim)
        out = pl.pallas_call(
            body,
            out_shape=jax.ShapeDtypeStruct((micro_n, seq_n, model_n), bf),
            in_specs=[sm, sm] + [hb] * 5 + [vm] * 8,
            out_specs=hb,
            scratch_shapes=[
                pltpu.VMEM((3, model_n, width_loc), bf),
                pltpu.VMEM((nc, width_loc, CH), bf),
                pltpu.VMEM((nu, model_n, CH), bf),
                pltpu.VMEM((nc, hid_loc, CH), bf),
                pltpu.VMEM((micro_n, nc, seq_n, CH), bf),
                pltpu.VMEM((2 * micro_n, nc, seq_n, CH), bf),
                pltpu.VMEM((2 * micro_n, nc, seq_n, CH), bf),
                pltpu.VMEM((2, nc, seq_n, CH), bf),
                pltpu.VMEM((seq_n, model_n), bf),
                pltpu.VMEM((seq_n, hid_loc), bf),
                pltpu.VMEM((3, seq_n, width_loc), bf),
                pltpu.VMEM((seq_n, width_loc), jnp.float32),
                pltpu.VMEM((seq_n, width_loc), bf),
                dma((3,)), dma((nc,)), dma((nu,)), dma((nc,)),
                dma((micro_n, nc)), dma((2 * micro_n, nc)), dma((2 * micro_n, nc)),
                dma((2 * micro_n, nc)), dma((2 * micro_n, nc)), dma((micro_n, nc)), dma((micro_n, nc)),
            ],
            compiler_params=pltpu.CompilerParams(
                collective_id=0, has_side_effects=True, vmem_limit_bytes=67043328),
            name='stages',
        )(
            seq_lens.reshape(micro_n), slopes,
            x_in.reshape(micro_n, seq_n, model_n),
            jnp.transpose(w_qkv[0], (1, 0, 2)), w_out[0], w_up[0], w_down[0],
            ln1_gain, ln1_shift, b_qkv.reshape(3, width_loc), b_out, ln2_gain, ln2_shift, b_up, b_down,
        )
        return out.reshape(1, micro_n, batch_n, seq_n, model_n)

    return jax.shard_map(per_device, mesh=mesh, in_specs=in_specs, out_specs=P('pp', 'dp'), check_vma=False)
```

```python
import functools
import math

import jax
import jax.numpy as jnp
from jax import lax
from jax.experimental import pallas as pl
from jax.experimental.pallas import tpu as pltpu
from jax.sharding import PartitionSpec as P

MESH = pl.DeviceIdType.MESH
CH = 256
WC = 512


def alibi_slopes(heads_n):
    closest = 2 ** int(math.floor(math.log2(heads_n)))
    base_rate = 2.0 ** (-8.0 / closest)
    slope_list = [base_rate ** (head_idx + 1) for head_idx in range(closest)]
    extra_rate = 2.0 ** (-4.0 / closest)
    slope_list = slope_list + [extra_rate ** (2 * head_idx + 1) for head_idx in range(min(closest, heads_n - closest))]
    return jnp.array(slope_list, dtype=jnp.float32)


def kernel(stages, micro_n, seq_n, model_n, hid_loc, heads_loc, head_dim,
           lens_ref, slopes_ref, x_hbm, wqkv_hbm, wout_hbm, wup_hbm, wdown_hbm,
           g1_ref, s1_ref, bqkv_ref, bo_ref, g2_ref, s2_ref, bup_ref, bd_ref,
           out_hbm,
           wqkv, wout, wup, wdown, xbuf, in1, in2, part, a_ref, u_ref, qkv, ctx, ctxb,
           wq_sem, wo_sem, wu_sem, wd_sem, x_sem, in1_sem, in2_sem, s1_sem, s2_sem, f_sem, o_sem):
    tp = lax.axis_index('tp')
    pp = lax.axis_index('pp')
    nc = model_n // CH
    nw = model_n // WC
    nu = hid_loc // WC
    sub = WC // CH
    inner = (tp == 1) | (tp == 2)
    outer = (tp == 0) | (tp == 3)
    partner = tp + 1 - 2 * (tp % 2)
    peer = 3 - tp
    first = pp == 0
    later = pp > 0
    sends = pp < stages - 1

    def x_copy(u, c):
        return pltpu.make_async_copy(x_hbm.at[u, :, pl.ds(c * CH, CH)], xbuf.at[u, c], x_sem.at[u, c])

    def wq_copy(c):
        return pltpu.make_async_copy(wqkv_hbm.at[c], wqkv.at[c], wq_sem.at[c])

    def wo_copy(c):
        return pltpu.make_async_copy(wout_hbm.at[:, pl.ds(c * WC, WC)], wout.at[c], wo_sem.at[c])

    def wu_copy(c):
        return pltpu.make_async_copy(wup_hbm.at[:, pl.ds(c * WC, WC)], wup.at[c], wu_sem.at[c])

    def wd_copy(c):
        return pltpu.make_async_copy(wdown_hbm.at[:, pl.ds(c * WC, WC)], wdown.at[c], wd_sem.at[c])

    @pl.when(first)
    def _():
        for c in range(nc):
            x_copy(0, c).start()
    for c in range(3):
        wq_copy(c).start()
    for c in range(nw):
        wo_copy(c).start()
    for c in range(nu):
        wu_copy(c).start()
    for c in range(nw):
        wd_copy(c).start()

    @pl.when(first)
    def _():
        for u in range(1, micro_n):
            for c in range(nc):
                x_copy(u, c).start()

    barrier = pltpu.get_barrier_semaphore()
    links = ((tp > 0, {'tp': tp - 1}), (tp < 3, {'tp': tp + 1}), (later, {'pp': pp - 1}), (sends, {'pp': pp + 1}))
    for cond, dev in links:
        @pl.when(cond)
        def _(dev=dev):
            pl.semaphore_signal(barrier, inc=1, device_id=dev, device_id_type=MESH)
    pl.semaphore_wait(barrier, sum(cond.astype(jnp.int32) for cond, _ in links))

    def part_copy(k, c):
        return pltpu.make_async_remote_copy(
            src_ref=part.at[k % 2, c], dst_ref=in1.at[k, c], send_sem=s1_sem.at[k, c], recv_sem=in1_sem.at[k, c],
            device_id={'tp': partner}, device_id_type=MESH)

    def sum_copy(k, c):
        return pltpu.make_async_remote_copy(
            src_ref=part.at[k % 2, c], dst_ref=in2.at[k, c], send_sem=s1_sem.at[k, c], recv_sem=in2_sem.at[k, c],
            device_id={'tp': peer}, device_id_type=MESH)

    def res_copy(k, c):
        return pltpu.make_async_remote_copy(
            src_ref=in1.at[k, c], dst_ref=in1.at[k, c], send_sem=s2_sem.at[k, c], recv_sem=in1_sem.at[k, c],
            device_id={'tp': partner}, device_id_type=MESH)

    def fwd_copy(u, c):
        return pltpu.make_async_remote_copy(
            src_ref=in1.at[2 * u + 1, c], dst_ref=xbuf.at[u, c], send_sem=f_sem.at[u, c], recv_sem=x_sem.at[u, c],
            device_id={'pp': pp + 1}, device_id_type=MESH)

    def out_copy(u, c):
        return pltpu.make_async_copy(in1.at[2 * u + 1, c], out_hbm.at[u, :, pl.ds(c * CH, CH)], o_sem.at[u, c])

    def cols(c, width=CH):
        return pl.ds(pl.multiple_of(c * width, width), width)

    rows_blk = 32

    def layer_norm(src, idx, gain, shift):
        @pl.loop(0, seq_n // rows_blk)
        def _(r):
            rows = pl.ds(pl.multiple_of(r * rows_blk, rows_blk), rows_blk)
            val = jnp.concatenate([src[idx, c, rows, :] for c in range(nc)], axis=-1).astype(jnp.float32)
            mean = jnp.sum(val, axis=-1, keepdims=True) * (1.0 / model_n)
            cen = val - mean
            var = jnp.sum(cen * cen, axis=-1, keepdims=True) * (1.0 / model_n)
            normed = cen * lax.rsqrt(var + 1e-5)
            a_ref[rows, :] = (normed * gain[...].astype(jnp.float32) + shift[...].astype(jnp.float32)).astype(jnp.bfloat16)

    def attention(u):
        seq_len = lens_ref[u]
        qpos = lax.broadcasted_iota(jnp.int32, (seq_n, seq_n), 0)
        kpos = lax.broadcasted_iota(jnp.int32, (seq_n, seq_n), 1)
        allowed = (kpos <= qpos) & (kpos < seq_len)
        dist = (qpos - kpos).astype(jnp.float32)
        ctx[...] = jnp.zeros_like(ctx)

        @pl.loop(0, heads_loc // 2)
        def _(g):
            win = pl.ds(pl.multiple_of(g * 128, 128), 256)
            lane = lax.broadcasted_iota(jnp.int32, (1, 256), 1) + g * 128
            low = 2 * head_dim * g
            m0 = ((lane >= low) & (lane < low + head_dim)).astype(jnp.float32).astype(jnp.bfloat16)
            m1 = ((lane >= low + head_dim) & (lane < low + 2 * head_dim)).astype(jnp.float32).astype(jnp.bfloat16)
            key = qkv[1, :, win]
            val = qkv[2, :, win]
            kk = jnp.concatenate([key * m0, key * m1], axis=0)
            vv = jnp.concatenate([val * m0, val * m1], axis=0)
            sc = lax.dot_general(qkv[0, :, win], kk, (((1,), (1,)), ((), ())), preferred_element_type=jnp.float32)
            probs = []
            for j in range(2):
                s = sc[:, j * seq_n:(j + 1) * seq_n] * (head_dim ** -0.5)
                s = s - slopes_ref[tp * heads_loc + 2 * g + j] * dist
                s = jnp.where(allowed, s, -1e30)
                e = jnp.exp(s - jnp.max(s, axis=-1, keepdims=True))
                probs.append((e / jnp.sum(e, axis=-1, keepdims=True)).astype(jnp.bfloat16))
            o = jnp.dot(jnp.concatenate(probs, axis=-1), vv, preferred_element_type=jnp.float32)
            ctx[:, win] += o
        ctxb[...] = ctx[...].astype(jnp.bfloat16)

    def own_partial(s, a, lhs, w, w_copy):
        k = 2 * s + a

        @pl.loop(0, nw)
        def _(w_idx):
            @pl.when(s == 0)
            def _():
                w_copy(w_idx).wait()

            @pl.when(s > 0)
            def _():
                for j in range(sub):
                    part_copy(k - 2, w_idx * sub + j).wait_send()
            val = jnp.dot(lhs[...], w[w_idx], preferred_element_type=jnp.float32).astype(jnp.bfloat16)
            for j in range(sub):
                part[a, w_idx * sub + j] = val[:, j * CH:(j + 1) * CH]

            @pl.when(outer)
            def _():
                for j in range(sub):
                    part_copy(k, w_idx * sub + j).start()

    def p1(s):
        for c in range(nc):
            x_copy(s, c).wait()
        layer_norm(xbuf, s, g1_ref, s1_ref)

        for c in range(3):
            @pl.when(s == 0)
            def _(c=c):
                wq_copy(c).wait()
            acc = jnp.dot(a_ref[...], wqkv[c], preferred_element_type=jnp.float32)
            qkv[c] = (acc + bqkv_ref[c:c + 1, :].astype(jnp.float32)).astype(jnp.bfloat16)
        attention(s)
        own_partial(s, 0, ctxb, wout, wo_copy)

    def p2(s):
        layer_norm(in1, 2 * s, g2_ref, s2_ref)

        @pl.loop(0, nu)
        def _(c):
            @pl.when(s == 0)
            def _():
                wu_copy(c).wait()
            t = jnp.dot(a_ref[...], wup[c], preferred_element_type=jnp.float32) + bup_ref[:, cols(c, WC)].astype(jnp.float32)
            t = 0.5 * t * (1.0 + jnp.tanh(math.sqrt(2.0 / math.pi) * (t + 0.044715 * (t * t * t))))
            u_ref[:, cols(c, WC)] = t.astype(jnp.bfloat16)
        own_partial(s, 1, u_ref, wdown, wd_copy)

    def r1(s, a):
        k = 2 * s + a

        @pl.when(inner)
        def _():
            @pl.loop(0, nc)
            def _(c):
                part_copy(k, c).wait_recv()
                part[a, c] = (part[a, c].astype(jnp.float32) + in1[k, c].astype(jnp.float32)).astype(jnp.bfloat16)
                sum_copy(k, c).start()

    def r2(s, a):
        k = 2 * s + a
        bias = bo_ref if a == 0 else bd_ref

        @pl.loop(0, nc)
        def _(c):
            @pl.when(inner)
            def _():
                sum_copy(k, c).wait_recv()
                resid = xbuf[s, c] if a == 0 else in1[2 * s, c]
                total = part[a, c].astype(jnp.float32) + in2[k, c].astype(jnp.float32)
                in1[k, c] = (resid.astype(jnp.float32) + total + bias[:, cols(c)].astype(jnp.float32)).astype(jnp.bfloat16)
                res_copy(k, c).start()

            @pl.when(outer)
            def _():
                part_copy(k, c).wait_recv()
            if a == 1:
                @pl.when(sends)
                def _():
                    fwd_copy(s, c).start()
                out_copy(s, c).start()

    @pl.loop(0, micro_n + 1)
    def _(s):
        @pl.when(s < micro_n)
        def _():
            p1(s)

        @pl.when(s > 0)
        def _():
            r1(s - 1, 1)
            r2(s - 1, 1)

        @pl.when(s < micro_n)
        def _():
            r1(s, 0)
            r2(s, 0)
            p2(s)

    last = micro_n - 1
    for a in range(2):
        for c in range(nc):
            part_copy(2 * last + a, c).wait_send()

    @pl.when(inner)
    def _():
        @pl.loop(0, 2 * micro_n)
        def _(k):
            @pl.loop(0, nc)
            def _(c):
                res_copy(k, c).wait_send()

    @pl.loop(0, micro_n)
    def _(u):
        @pl.loop(0, nc)
        def _(c):
            @pl.when(sends)
            def _():
                fwd_copy(u, c).wait_send()
            out_copy(u, c).wait()


def solution(mesh):
    stages = mesh.shape['pp']
    in_specs = (P('dp'), P('dp'), P('pp'), P('pp'), P('pp', None, None, 'tp'), P('pp', None, 'tp', None), P('pp', 'tp', None), P('pp'), P('pp'), P('pp'), P('pp', None, 'tp'), P('pp', 'tp'), P('pp', 'tp', None), P('pp'))

    def per_device(x_in, seq_lens, ln1_gain, ln1_shift, w_qkv, b_qkv, w_out, b_out, ln2_gain, ln2_shift, w_up, b_up, w_down, b_down):
        micro_n, batch_n, seq_n, model_n = x_in.shape
        heads_loc, head_dim = b_qkv.shape[2], b_qkv.shape[3]
        width_loc = heads_loc * head_dim
        hid_loc = w_up.shape[2]
        nc, nw, nu = model_n // CH, model_n // WC, hid_loc // WC
        assert batch_n == 1 and mesh.shape['tp'] == 4 and seq_n == 128
        slopes = alibi_slopes(heads_loc * mesh.shape['tp'])
        bf = jnp.bfloat16
        vm = pl.BlockSpec(memory_space=pltpu.VMEM)
        sm = pl.BlockSpec(memory_space=pltpu.SMEM)
        hb = pl.BlockSpec(memory_space=pl.ANY)
        dma = pltpu.SemaphoreType.DMA
        body = functools.partial(kernel, stages, micro_n, seq_n, model_n, hid_loc, heads_loc, head_dim)
        out = pl.pallas_call(
            body,
            out_shape=jax.ShapeDtypeStruct((micro_n, seq_n, model_n), bf),
            in_specs=[sm, sm] + [hb] * 5 + [vm] * 8,
            out_specs=hb,
            scratch_shapes=[
                pltpu.VMEM((3, model_n, width_loc), bf),
                pltpu.VMEM((nw, width_loc, WC), bf),
                pltpu.VMEM((nu, model_n, WC), bf),
                pltpu.VMEM((nw, hid_loc, WC), bf),
                pltpu.VMEM((micro_n, nc, seq_n, CH), bf),
                pltpu.VMEM((2 * micro_n, nc, seq_n, CH), bf),
                pltpu.VMEM((2 * micro_n, nc, seq_n, CH), bf),
                pltpu.VMEM((2, nc, seq_n, CH), bf),
                pltpu.VMEM((seq_n, model_n), bf),
                pltpu.VMEM((seq_n, hid_loc), bf),
                pltpu.VMEM((3, seq_n, width_loc), bf),
                pltpu.VMEM((seq_n, width_loc), jnp.float32),
                pltpu.VMEM((seq_n, width_loc), bf),
                dma((3,)), dma((nw,)), dma((nu,)), dma((nw,)),
                dma((micro_n, nc)), dma((2 * micro_n, nc)), dma((2 * micro_n, nc)),
                dma((2 * micro_n, nc)), dma((2 * micro_n, nc)), dma((micro_n, nc)), dma((micro_n, nc)),
            ],
            compiler_params=pltpu.CompilerParams(
                collective_id=0, has_side_effects=True, vmem_limit_bytes=67043328),
            name='stages',
        )(
            seq_lens.reshape(micro_n), slopes,
            x_in.reshape(micro_n, seq_n, model_n),
            jnp.transpose(w_qkv[0], (1, 0, 2)), w_out[0], w_up[0], w_down[0],
            ln1_gain, ln1_shift, b_qkv.reshape(3, width_loc), b_out, ln2_gain, ln2_shift, b_up, b_down,
        )
        return out.reshape(1, micro_n, batch_n, seq_n, model_n)

    return jax.shard_map(per_device, mesh=mesh, in_specs=in_specs, out_specs=P('pp', 'dp'), check_vma=False)
```

```python
import functools
import math

import jax
import jax.numpy as jnp
from jax import lax
from jax.experimental import pallas as pl
from jax.experimental.pallas import tpu as pltpu
from jax.sharding import PartitionSpec as P

MESH = pl.DeviceIdType.MESH
CH = 512
WC = 512


def alibi_slopes(heads_n):
    closest = 2 ** int(math.floor(math.log2(heads_n)))
    base_rate = 2.0 ** (-8.0 / closest)
    slope_list = [base_rate ** (head_idx + 1) for head_idx in range(closest)]
    extra_rate = 2.0 ** (-4.0 / closest)
    slope_list = slope_list + [extra_rate ** (2 * head_idx + 1) for head_idx in range(min(closest, heads_n - closest))]
    return jnp.array(slope_list, dtype=jnp.float32)


TOK = 64
TABLES = {
    (0, 0): (
        2048, 18440, 34832, 274438, 798982, 4614, 28675, 553102, 1077646, 45066, 569494, 831499, 37398, 14355,
        538759, 1063303, 51224, 292879, 817423, 66063, 67607, 571543, 1096087, 84008, 323614, 848158, 53790, 55334,
        602278, 1126822, 94242, 356387, 880942, 86574, 88095, 587935, 1112479, 79920, 342065, 866599, 115239, 116783,
        620719, 1145263, 372790, 897334, 102966, 127027, 651454, 1175998, 120890, 374839, 899383, 129591, 653503, 1178047,
        3934080, 3934080, 3934080, 3934080, 3934080, 3934080, 3934080, 3934080, 3934080, 3934080, 3934080, 3934080, 3934080, 3934080,
        3934080, 3934080, 3934080, 3934080, 3934080, 3934080, 3934080, 3934080, 3934080, 3934080, 3934080, 3934080, 3934080, 3934080,
        3934080, 3934080, 3934080, 3934080, 3934080, 3934080, 3934080, 3934080, 3934080, 3934080, 3934080, 3934080,
    ),
    (0, 1): (
        2048, 18440, 8208, 532612, 35204, 25092, 549004, 811014, 1073286, 41222, 303494, 565766, 28674, 553102,
        1077646, 307222, 569748, 6676, 831498, 10774, 272395, 796933, 37381, 38919, 538759, 27015, 289287, 813325,
        49677, 30741, 567445, 829583, 1091855, 51599, 47631, 309280, 833815, 68119, 319516, 581672, 84380, 1105950,
        73886, 336158, 598430, 53790, 860198, 1122470, 55340, 352550, 864556, 877094, 94242, 1138862, 618531, 321565,
        584110, 86574, 845855, 326173, 587819, 337957, 850213, 1112485, 79920, 1124519, 100397, 354599, 866605, 1128877,
        96312, 358957, 620601, 368692, 631215, 893487, 1155126, 635062, 897084, 1159356, 647218, 127420, 389171, 651836,
        1175998, 108602, 121013, 895285, 113205, 637111, 1161655, 387133, 129341, 1173949, 653503, 1178047,
    ),
    (1, 0): (
        2048, 18440, 34832, 274438, 798982, 4614, 28675, 553102, 1077646, 22538, 307222, 831766, 1093639, 276498,
        538643, 1063303, 292879, 555032, 51599, 47631, 309280, 571425, 1096087, 61480, 323625, 848158, 53790, 55334,
        602278, 1126822, 94242, 356387, 880942, 86574, 63531, 587935, 98719, 80415, 342065, 866599, 96807, 620719,
        1145263, 110648, 116918, 897334, 102966, 127027, 651454, 1175998, 120890, 374839, 899383, 129591, 653503, 1178047,
        3934080, 3934080, 3934080, 3934080, 3934080, 3934080, 3934080, 3934080, 3934080, 3934080, 3934080, 3934080, 3934080, 3934080,
        3934080, 3934080, 3934080, 3934080, 3934080, 3934080, 3934080, 3934080, 3934080, 3934080, 3934080, 3934080, 3934080, 3934080,
        3934080, 3934080, 3934080, 3934080, 3934080, 3934080, 3934080, 3934080, 3934080, 3934080, 3934080, 3934080,
    ),
    (1, 1): (
        2048, 18440, 8208, 34948, 794884, 12804, 274444, 536716, 798988, 1061260, 28674, 1073294, 41230, 815252,
        565251, 1077652, 45066, 10390, 23060, 831766, 534661, 796679, 37398, 276997, 38925, 801031, 551053, 1063309,
        31245, 49295, 817423, 305173, 51727, 829717, 1091607, 309280, 67863, 57751, 320023, 82204, 323614, 1106332,
        585769, 335908, 598430, 1110436, 77850, 602278, 90660, 864428, 876844, 1126427, 70188, 356398, 880942, 59950,
        321571, 846109, 86557, 75807, 325675, 850207, 338463, 600103, 98725, 342565, 100397, 354599, 866605, 1141165,
        96807, 358452, 620724, 882996, 1145268, 110648, 635062, 1155510, 1159225, 104498, 385084, 909628, 127548, 651454,
        913461, 1175733, 119093, 374839, 637365, 121397, 1161655, 387133, 911677, 129597, 653503, 1178047,
    ),
    (2, 0): (
        2048, 18440, 274438, 536592, 35206, 4614, 28675, 553102, 1077646, 22538, 307222, 831766, 1093639, 38930,
        538759, 1063303, 292879, 49423, 51599, 66063, 47137, 571543, 833576, 84503, 323614, 848158, 53790, 77851,
        602278, 1126822, 71714, 356398, 880942, 1142832, 63537, 88106, 114847, 117023, 1112479, 342055, 866599, 111143,
        635062, 96694, 620719, 102966, 104879, 127535, 651454, 1175998, 120890, 374839, 899383, 129591, 653503, 1178047,
        3934080, 3934080, 3934080, 3934080, 3934080, 3934080, 3934080, 3934080, 3934080, 3934080, 3934080, 3934080, 3934080, 3934080,
        3934080, 3934080, 3934080, 3934080, 3934080, 3934080, 3934080, 3934080, 3934080, 3934080, 3934080, 3934080, 3934080, 3934080,
        3934080, 3934080, 3934080, 3934080, 3934080, 3934080, 3934080, 3934080, 3934080, 3934080, 3934080, 3934080,
    ),
    (2, 1): (
        2048, 18440, 270340, 794884, 12804, 32902, 798982, 25094, 286722, 811276, 6668, 34830, 553102, 41358,
        21006, 565396, 10644, 45588, 22661, 796933, 1058966, 831766, 1093639, 276498, 801031, 27143, 551053, 1075597,
        30739, 555151, 817176, 43535, 567445, 51605, 66069, 309271, 833815, 68119, 57384, 581788, 1106332, 61481,
        323620, 336158, 1110430, 53540, 860198, 90660, 352422, 55596, 876838, 864812, 70182, 356398, 59694, 72110,
        322094, 583722, 845855, 88605, 98463, 76063, 100517, 600479, 1112485, 115237, 342055, 368692, 893236, 92455,
        354727, 616999, 879156, 110649, 1140918, 123190, 96694, 358588, 620860, 102966, 909743, 1172015, 127027, 651454,
        1175998, 108602, 121013, 895285, 113205, 637111, 1161655, 387133, 911677, 1173567, 653503, 1178047,
    ),
    (3, 0): (
        2048, 18440, 274438, 798982, 4614, 6160, 28689, 553102, 1077646, 22538, 276487, 801031, 45575, 569494,
        1094038, 30738, 292883, 817423, 1079320, 65561, 47137, 571543, 61847, 1095720, 323625, 848158, 53790, 340006,
        55590, 1126822, 71714, 98350, 100526, 880942, 86574, 88095, 587935, 1112479, 114727, 604327, 117159, 111143,
        96438, 620719, 897334, 1159599, 127026, 105007, 651454, 1175998, 120890, 374839, 899383, 129591, 653503, 1178047,
        3934080, 3934080, 3934080, 3934080, 3934080, 3934080, 3934080, 3934080, 3934080, 3934080, 3934080, 3934080, 3934080, 3934080,
        3934080, 3934080, 3934080, 3934080, 3934080, 3934080, 3934080, 3934080, 3934080, 3934080, 3934080, 3934080, 3934080, 3934080,
        3934080, 3934080, 3934080, 3934080, 3934080, 3934080, 3934080, 3934080, 3934080, 3934080, 3934080, 3934080,
    ),
    (3, 1): (
        2048, 18440, 270340, 794884, 12804, 32902, 798982, 35334, 24578, 549004, 811011, 29196, 553102, 10638,
        21006, 534661, 1059205, 14356, 303115, 565383, 801031, 1063316, 45588, 307213, 569485, 831757, 1094029, 30738,
        1075343, 555027, 49551, 51727, 65557, 67733, 47381, 1091989, 57495, 571548, 844060, 1106327, 61480, 74263,
        323748, 860452, 84516, 848158, 53790, 340006, 864550, 55846, 90146, 614572, 1139116, 94243, 356400, 880942,
        321565, 584238, 86429, 64029, 337957, 862501, 1124511, 88351, 1112479, 100391, 604327, 106919, 92711, 368813,
        631085, 879028, 1141300, 114742, 96438, 620719, 117046, 883126, 1159228, 1145020, 127026, 909628, 1171646, 651315,
        1175998, 120890, 370741, 895285, 113205, 637111, 899133, 1161405, 911677, 129597, 653503, 1178047,
    ),
}


def kernel(stages, micro_n, seq_n, model_n, hid_loc, heads_loc, head_dim,
           lens_ref, slopes_ref, x_hbm, wqkv_hbm, wout_hbm, wup_hbm, wdown_hbm,
           g1_ref, s1_ref, bqkv_ref, bo_ref, g2_ref, s2_ref, bup_ref, bd_ref,
           out_hbm,
           wqkv, wout, wup, wdown, xbuf, in1, in2, part, a_ref, u_ref, q_ref, kv_ref, ctx, ctxb,
           wq_sem, wo_sem, wu_sem, wd_sem, x_sem, in1_sem, in2_sem, s1_sem, s2_sem, f_sem, o_sem):
    tp = lax.axis_index('tp')
    pp = lax.axis_index('pp')
    nc = model_n // CH
    nw = model_n // WC
    nu = hid_loc // WC
    sub = WC // CH
    halves = seq_n // TOK
    units = micro_n * halves
    inner = (tp == 1) | (tp == 2)
    outer = (tp == 0) | (tp == 3)
    partner = tp + 1 - 2 * (tp % 2)
    peer = 3 - tp
    first = pp == 0
    later = pp > 0
    sends = pp < stages - 1

    def where(u):
        return lax.div(u, halves), pl.ds(pl.multiple_of(lax.rem(u, halves) * TOK, TOK), TOK)

    def x_copy(u, c):
        m, rows = where(u)
        return pltpu.make_async_copy(x_hbm.at[m, rows, pl.ds(c * CH, CH)], xbuf.at[u, c], x_sem.at[u, c])

    def wq_copy(c):
        return pltpu.make_async_copy(wqkv_hbm.at[c], wqkv.at[c], wq_sem.at[c])

    def wo_copy(c):
        return pltpu.make_async_copy(wout_hbm.at[:, pl.ds(c * WC, WC)], wout.at[c], wo_sem.at[c])

    def wu_copy(c):
        return pltpu.make_async_copy(wup_hbm.at[:, pl.ds(c * WC, WC)], wup.at[c], wu_sem.at[c])

    def wd_copy(c):
        return pltpu.make_async_copy(wdown_hbm.at[:, pl.ds(c * WC, WC)], wdown.at[c], wd_sem.at[c])

    @pl.when(first)
    def _():
        for c in range(nc):
            x_copy(jnp.int32(0), c).start()
    for c in range(3):
        wq_copy(c).start()
    for c in range(nw):
        wo_copy(c).start()
    for c in range(nu):
        wu_copy(c).start()
    for c in range(nw):
        wd_copy(c).start()

    @pl.when(first)
    def _():
        @pl.loop(1, units)
        def _(u):
            for c in range(nc):
                x_copy(u, c).start()

    barrier = pltpu.get_barrier_semaphore()
    links = ((tp > 0, {'tp': tp - 1}), (tp < 3, {'tp': tp + 1}), (later, {'pp': pp - 1}), (sends, {'pp': pp + 1}))
    for cond, dev in links:
        @pl.when(cond)
        def _(dev=dev):
            pl.semaphore_signal(barrier, inc=1, device_id=dev, device_id_type=MESH)
    mine = [(((pp == stage) & (inner if role else outer)).astype(jnp.int32), words) for (stage, role), words in TABLES.items()]
    table = [sum(sel * words[j] for sel, words in mine) for j in range(len(TABLES[0, 0]))]
    pl.semaphore_wait(barrier, sum(cond.astype(jnp.int32) for cond, _ in links))

    def part_copy(k, c):
        return pltpu.make_async_remote_copy(
            src_ref=part.at[k, c], dst_ref=in1.at[k, c], send_sem=s1_sem.at[k, c], recv_sem=in1_sem.at[k, c],
            device_id={'tp': partner}, device_id_type=MESH)

    def sum_copy(k, c):
        return pltpu.make_async_remote_copy(
            src_ref=part.at[k, c], dst_ref=in2.at[k, c], send_sem=s1_sem.at[k, c], recv_sem=in2_sem.at[k, c],
            device_id={'tp': peer}, device_id_type=MESH)

    def res_copy(k, c):
        return pltpu.make_async_remote_copy(
            src_ref=in1.at[k, c], dst_ref=in1.at[k, c], send_sem=s2_sem.at[k, c], recv_sem=in1_sem.at[k, c],
            device_id={'tp': partner}, device_id_type=MESH)

    def fwd_copy(u, c):
        return pltpu.make_async_remote_copy(
            src_ref=in1.at[2 * u + 1, c], dst_ref=xbuf.at[u, c], send_sem=f_sem.at[u, c], recv_sem=x_sem.at[u, c],
            device_id={'pp': pp + 1}, device_id_type=MESH)

    def out_copy(u, c):
        m, rows = where(u)
        return pltpu.make_async_copy(
            in1.at[2 * u + 1, c], out_hbm.at[m, rows, pl.ds(pl.multiple_of(c * CH, CH), CH)], o_sem.at[u, c])

    def cols(c, width=CH):
        return pl.ds(pl.multiple_of(c * width, width), width)

    rows_blk = 32

    def layer_norm(src, idx, gain, shift):
        @pl.loop(0, TOK // rows_blk)
        def _(r):
            rows = pl.ds(pl.multiple_of(r * rows_blk, rows_blk), rows_blk)
            val = jnp.concatenate([src[idx, c, rows, :] for c in range(nc)], axis=-1).astype(jnp.float32)
            mean = jnp.sum(val, axis=-1, keepdims=True) * (1.0 / model_n)
            cen = val - mean
            var = jnp.sum(cen * cen, axis=-1, keepdims=True) * (1.0 / model_n)
            normed = cen * lax.rsqrt(var + 1e-5)
            a_ref[rows, :] = (normed * gain[...].astype(jnp.float32) + shift[...].astype(jnp.float32)).astype(jnp.bfloat16)

    def attention(u):
        m = lax.div(u, halves)
        seq_len = lens_ref[m]
        qpos = lax.broadcasted_iota(jnp.int32, (TOK, seq_n), 0) + lax.rem(u, halves) * TOK
        kpos = lax.broadcasted_iota(jnp.int32, (TOK, seq_n), 1)
        allowed = (kpos <= qpos) & (kpos < seq_len)
        dist = (qpos - kpos).astype(jnp.float32)
        ctx[...] = jnp.zeros_like(ctx)

        @pl.loop(0, heads_loc // 2)
        def _(g):
            win = pl.ds(pl.multiple_of(g * 128, 128), 256)
            lane = lax.broadcasted_iota(jnp.int32, (1, 256), 1) + g * 128
            low = 2 * head_dim * g
            m0 = ((lane >= low) & (lane < low + head_dim)).astype(jnp.float32).astype(jnp.bfloat16)
            m1 = ((lane >= low + head_dim) & (lane < low + 2 * head_dim)).astype(jnp.float32).astype(jnp.bfloat16)
            key = kv_ref[0, :, win]
            val = kv_ref[1, :, win]
            kk = jnp.concatenate([key * m0, key * m1], axis=0)
            vv = jnp.concatenate([val * m0, val * m1], axis=0)
            sc = lax.dot_general(q_ref[:, win], kk, (((1,), (1,)), ((), ())), preferred_element_type=jnp.float32)
            probs = []
            for j in range(2):
                s = sc[:, j * seq_n:(j + 1) * seq_n] * (head_dim ** -0.5)
                s = s - slopes_ref[tp * heads_loc + 2 * g + j] * dist
                s = jnp.where(allowed, s, -1e30)
                e = jnp.exp(s - jnp.max(s, axis=-1, keepdims=True))
                probs.append((e / jnp.sum(e, axis=-1, keepdims=True)).astype(jnp.bfloat16))
            o = jnp.dot(jnp.concatenate(probs, axis=-1), vv, preferred_element_type=jnp.float32)
            ctx[:, win] += o
        ctxb[...] = ctx[...].astype(jnp.bfloat16)

    def own_partial(u, a, lhs, w, w_copy):
        k = 2 * u + a

        @pl.loop(0, nw)
        def _(w_idx):
            @pl.when(u == 0)
            def _():
                w_copy(w_idx).wait()
            val = jnp.dot(lhs[...], w[w_idx], preferred_element_type=jnp.float32).astype(jnp.bfloat16)
            for j in range(sub):
                part[k, w_idx * sub + j] = val[:, j * CH:(j + 1) * CH]

            @pl.when(outer)
            def _():
                for j in range(sub):
                    part_copy(k, w_idx * sub + j).start()

    def p1a(u):
        _, rows = where(u)
        for c in range(nc):
            x_copy(u, c).wait()
        layer_norm(xbuf, u, g1_ref, s1_ref)
        if halves > 1:
            @pl.when(lax.rem(u, halves) == 0)
            def _():
                kv_ref[:, TOK:, :] = jnp.zeros((2, seq_n - TOK, kv_ref.shape[2]), kv_ref.dtype)
        for c in range(3):
            @pl.when(u == 0)
            def _(c=c):
                wq_copy(c).wait()
            acc = jnp.dot(a_ref[...], wqkv[c], preferred_element_type=jnp.float32)
            acc = (acc + bqkv_ref[c:c + 1, :].astype(jnp.float32)).astype(jnp.bfloat16)
            if c == 0:
                q_ref[...] = acc
            else:
                kv_ref[c - 1, rows, :] = acc

    def p1b(u):
        attention(u)
        own_partial(u, 0, ctxb, wout, wo_copy)

    def p2a(u):
        layer_norm(in1, 2 * u, g2_ref, s2_ref)

        @pl.loop(0, nu)
        def _(c):
            @pl.when(u == 0)
            def _():
                wu_copy(c).wait()
            t = jnp.dot(a_ref[...], wup[c], preferred_element_type=jnp.float32) + bup_ref[:, cols(c, WC)].astype(jnp.float32)
            t = 0.5 * t * (1.0 + jnp.tanh(math.sqrt(2.0 / math.pi) * (t + 0.044715 * (t * t * t))))
            u_ref[:, cols(c, WC)] = t.astype(jnp.bfloat16)

    def p2b(u):
        own_partial(u, 1, u_ref, wdown, wd_copy)

    def r1(u, a, c):
        k = 2 * u + a
        part_copy(k, c).wait_recv()
        part[k, c] = (part[k, c].astype(jnp.float32) + in1[k, c].astype(jnp.float32)).astype(jnp.bfloat16)
        sum_copy(k, c).start()

    def r2(u, a, c):
        k = 2 * u + a
        bias = bo_ref if a == 0 else bd_ref

        @pl.when(inner)
        def _():
            sum_copy(k, c).wait_recv()
            resid = xbuf[u, c] if a == 0 else in1[2 * u, c]
            total = part[k, c].astype(jnp.float32) + in2[k, c].astype(jnp.float32)
            in1[k, c] = (resid.astype(jnp.float32) + total + bias[:, cols(c)].astype(jnp.float32)).astype(jnp.bfloat16)
            res_copy(k, c).start()

        @pl.when(outer)
        def _():
            part_copy(k, c).wait_recv()
        if a == 1:
            @pl.when(sends)
            def _():
                fwd_copy(u, c).start()
            out_copy(u, c).start()

    ops = (p1a, p1b, p2a, p2b)

    def step(_, word):
        entry = lax.rem(word, 2048)
        op, u, c = lax.rem(entry, 8), lax.rem(lax.div(entry, 8), 16), lax.div(entry, 128)

        @pl.when(op < 4)
        def _():
            for i, fn in enumerate(ops):
                @pl.when((op == i) & (c == 0))
                def _(fn=fn):
                    fn(u)

        @pl.when(op >= 4)
        def _():
            for a in range(2):
                @pl.when(op == 4 + a)
                def _(a=a):
                    r1(u, a, c)

                @pl.when(op == 6 + a)
                def _(a=a):
                    r2(u, a, c)
        return lax.div(word, 2048)

    @pl.loop(0, len(TABLES[0, 0]))
    def _(t):
        lax.fori_loop(0, 2, step, sum((t == j).astype(jnp.int32) * word for j, word in enumerate(table)))

    @pl.loop(0, 2 * units)
    def _(k):
        for c in range(nc):
            part_copy(k, c).wait_send()

        @pl.when(inner)
        def _():
            for c in range(nc):
                res_copy(k, c).wait_send()

    @pl.loop(0, units)
    def _(u):
        @pl.when(sends)
        def _():
            for c in range(nc):
                fwd_copy(u, c).wait_send()
        for c in range(nc):
            out_copy(u, c).wait()


def solution(mesh):
    stages = mesh.shape['pp']
    in_specs = (P('dp'), P('dp'), P('pp'), P('pp'), P('pp', None, None, 'tp'), P('pp', None, 'tp', None), P('pp', 'tp', None), P('pp'), P('pp'), P('pp'), P('pp', None, 'tp'), P('pp', 'tp'), P('pp', 'tp', None), P('pp'))

    def per_device(x_in, seq_lens, ln1_gain, ln1_shift, w_qkv, b_qkv, w_out, b_out, ln2_gain, ln2_shift, w_up, b_up, w_down, b_down):
        micro_n, batch_n, seq_n, model_n = x_in.shape
        heads_loc, head_dim = b_qkv.shape[2], b_qkv.shape[3]
        width_loc = heads_loc * head_dim
        hid_loc = w_up.shape[2]
        nc, nw, nu = model_n // CH, model_n // WC, hid_loc // WC
        units = micro_n * seq_n // TOK
        assert batch_n == 1 and mesh.shape['tp'] == 4 and seq_n == 128
        slopes = alibi_slopes(heads_loc * mesh.shape['tp'])
        bf = jnp.bfloat16
        vm = pl.BlockSpec(memory_space=pltpu.VMEM)
        sm = pl.BlockSpec(memory_space=pltpu.SMEM)
        hb = pl.BlockSpec(memory_space=pl.ANY)
        dma = pltpu.SemaphoreType.DMA
        body = functools.partial(kernel, stages, micro_n, seq_n, model_n, hid_loc, heads_loc, head_dim)
        out = pl.pallas_call(
            body,
            out_shape=jax.ShapeDtypeStruct((micro_n, seq_n, model_n), bf),
            in_specs=[sm, sm] + [hb] * 5 + [vm] * 8,
            out_specs=hb,
            scratch_shapes=[
                pltpu.VMEM((3, model_n, width_loc), bf),
                pltpu.VMEM((nw, width_loc, WC), bf),
                pltpu.VMEM((nu, model_n, WC), bf),
                pltpu.VMEM((nw, hid_loc, WC), bf),
                pltpu.VMEM((units, nc, TOK, CH), bf),
                pltpu.VMEM((2 * units, nc, TOK, CH), bf),
                pltpu.VMEM((2 * units, nc, TOK, CH), bf),
                pltpu.VMEM((2 * units, nc, TOK, CH), bf),
                pltpu.VMEM((TOK, model_n), bf),
                pltpu.VMEM((TOK, hid_loc), bf),
                pltpu.VMEM((TOK, width_loc), bf),
                pltpu.VMEM((2, seq_n, width_loc), bf),
                pltpu.VMEM((TOK, width_loc), jnp.float32),
                pltpu.VMEM((TOK, width_loc), bf),
                dma((3,)), dma((nw,)), dma((nu,)), dma((nw,)),
                dma((units, nc)), dma((2 * units, nc)), dma((2 * units, nc)),
                dma((2 * units, nc)), dma((2 * units, nc)), dma((units, nc)), dma((units, nc)),
            ],
            compiler_params=pltpu.CompilerParams(
                collective_id=0, has_side_effects=True, vmem_limit_bytes=67043328),
            name='stages',
        )(
            seq_lens.reshape(micro_n), slopes,
            x_in.reshape(micro_n, seq_n, model_n),
            jnp.transpose(w_qkv[0], (1, 0, 2)), w_out[0], w_up[0], w_down[0],
            ln1_gain, ln1_shift, b_qkv.reshape(3, width_loc), b_out, ln2_gain, ln2_shift, b_up, b_down,
        )
        return out.reshape(1, micro_n, batch_n, seq_n, model_n)

    return jax.shard_map(per_device, mesh=mesh, in_specs=in_specs, out_specs=P('pp', 'dp'), check_vma=False)
```

```python
import functools
import math

import jax
import jax.numpy as jnp
from jax import lax
from jax.experimental import pallas as pl
from jax.experimental.pallas import tpu as pltpu
from jax.sharding import PartitionSpec as P

MESH = pl.DeviceIdType.MESH
CH = 512
WC = 512


def alibi_slopes(heads_n):
    closest = 2 ** int(math.floor(math.log2(heads_n)))
    base_rate = 2.0 ** (-8.0 / closest)
    slope_list = [base_rate ** (head_idx + 1) for head_idx in range(closest)]
    extra_rate = 2.0 ** (-4.0 / closest)
    slope_list = slope_list + [extra_rate ** (2 * head_idx + 1) for head_idx in range(min(closest, heads_n - closest))]
    return jnp.array(slope_list, dtype=jnp.float32)


TOK = 64
TABLES = {
    (0, 0): (
        2048, 18440, 34832, 51224, 67616, 274438, 798982, 4614, 815246, 6158, 1077518, 45066, 22806, 1094038,
        37014, 323614, 1110302, 847891, 55322, 276487, 801031, 82439, 30761, 555151, 1079695, 602160, 77990, 864305,
        1126423, 309282, 571427, 1096087, 325688, 849977, 64031, 587822, 618670, 1143214, 110634, 372779, 897334, 102966,
        104487, 604327, 1128871, 389182, 913726, 119358, 120879, 620719, 1145263, 374839, 899383, 129591, 653503, 1178047,
        3934080, 3934080, 3934080, 3934080, 3934080, 3934080, 3934080, 3934080, 3934080, 3934080, 3934080, 3934080, 3934080, 3934080,
        3934080, 3934080, 3934080, 3934080, 3934080, 3934080, 3934080, 3934080, 3934080, 3934080, 3934080, 3934080, 3934080, 3934080,
        3934080, 3934080, 3934080, 3934080, 3934080, 3934080, 3934080, 3934080, 3934080, 3934080, 3934080, 3934080,
    ),
    (0, 1): (
        2048, 18440, 8208, 34948, 794884, 1056792, 286732, 548870, 274457, 811270, 1073542, 65556, 29190, 303246,
        553236, 1089940, 57742, 1077404, 45058, 307484, 831766, 844310, 61980, 323587, 20766, 272389, 534942, 23070,
        1059205, 26657, 14477, 550948, 336007, 539021, 1075492, 860551, 1063460, 30738, 77967, 555027, 305173, 829717,
        817685, 340495, 864550, 47130, 55846, 59543, 583837, 833815, 1108381, 70167, 63528, 71839, 84255, 850463,
        352300, 876844, 98860, 106545, 630964, 1155508, 94245, 337976, 618670, 600121, 1143214, 862250, 111141, 372779,
        634940, 897212, 1159484, 79922, 1171900, 342067, 1128743, 92583, 127149, 389421, 651693, 913965, 1175605, 118965,
        96565, 895035, 1157295, 882991, 113199, 637111, 899133, 1161405, 911677, 1173567, 653503, 1178047,
    ),
    (1, 0): (
        2048, 18440, 12304, 274449, 798982, 4614, 290830, 552963, 51224, 1077646, 45066, 307211, 831766, 37398,
        14355, 538759, 1063303, 61472, 323617, 848158, 53790, 55311, 555151, 82319, 84495, 309271, 833815, 1095728,
        340017, 78118, 1126822, 63522, 71839, 850207, 1112120, 356398, 618553, 1143214, 110634, 634923, 1159606, 102582,
        342055, 604211, 1128871, 127023, 651454, 620719, 883134, 119358, 113199, 374843, 899383, 129591, 653503, 1178047,
        3934080, 3934080, 3934080, 3934080, 3934080, 3934080, 3934080, 3934080, 3934080, 3934080, 3934080, 3934080, 3934080, 3934080,
        3934080, 3934080, 3934080, 3934080, 3934080, 3934080, 3934080, 3934080, 3934080, 3934080, 3934080, 3934080, 3934080, 3934080,
        3934080, 3934080, 3934080, 3934080, 3934080, 3934080, 3934080, 3934080, 3934080, 3934080, 3934080, 3934080,
    ),
    (1, 1): (
        2048, 18440, 270340, 12304, 794884, 274449, 25092, 286982, 1061254, 4364, 290830, 1073548, 552963, 49172,
        815252, 1077273, 20756, 827414, 307732, 569355, 272389, 831749, 1094021, 14354, 1058844, 319623, 538643, 844060,
        1106311, 27143, 61472, 67725, 585886, 551309, 1075614, 53790, 305173, 55311, 829717, 293397, 73999, 336271,
        1079588, 82340, 1122327, 83997, 309527, 833693, 584215, 845872, 78365, 100518, 90406, 614572, 876966, 1126956,
        63522, 587935, 849955, 1112110, 356404, 114868, 880942, 631342, 892982, 373300, 86073, 337957, 635173, 897445,
        1124918, 79915, 385084, 647335, 92210, 866599, 1128621, 127277, 909502, 651693, 1141308, 96307, 358453, 913711,
        633013, 895407, 119358, 1145397, 374839, 121143, 1161655, 387133, 911677, 129597, 653503, 1178047,
    ),
    (2, 0): (
        2048, 274438, 536584, 18822, 4614, 32771, 28689, 553102, 815128, 1077273, 20487, 538759, 800779, 45575,
        569494, 1094038, 38930, 67616, 323614, 848158, 53790, 292879, 81947, 84367, 1079344, 47153, 309519, 833815,
        78359, 114854, 864287, 117030, 587935, 1126815, 618530, 94751, 356387, 1143214, 88106, 897206, 110782, 635446,
        127026, 651315, 80318, 119358, 342075, 604711, 96679, 620719, 1145263, 374839, 899383, 129591, 653503, 1178047,
        3934080, 3934080, 3934080, 3934080, 3934080, 3934080, 3934080, 3934080, 3934080, 3934080, 3934080, 3934080, 3934080, 3934080,
        3934080, 3934080, 3934080, 3934080, 3934080, 3934080, 3934080, 3934080, 3934080, 3934080, 3934080, 3934080, 3934080, 3934080,
        3934080, 3934080, 3934080, 3934080, 3934080, 3934080, 3934080, 3934080, 3934080, 3934080, 3934080, 3934080,
    ),
    (2, 1): (
        2048, 270340, 794884, 16900, 274438, 18694, 1061254, 6146, 34832, 286732, 811276, 10764, 272398, 534670,
        49422, 1059205, 815111, 277006, 303124, 565511, 51604, 21012, 1063303, 307222, 569355, 1094038, 57362, 39068,
        844060, 66076, 288781, 61709, 323981, 585761, 848397, 53790, 292879, 55567, 305173, 82319, 829717, 1079829,
        73769, 335895, 309540, 98724, 571421, 321943, 1096228, 78109, 845873, 340509, 864550, 90143, 325804, 114988,
        850207, 877094, 1139231, 94260, 356386, 368942, 71988, 1143214, 1155508, 116790, 372778, 634940, 88252, 647606,
        1159612, 75826, 1171518, 337971, 651454, 913701, 80293, 1176101, 92218, 342189, 121127, 866605, 1128877, 96813,
        358453, 620725, 882997, 1145269, 113205, 374845, 637117, 899389, 1161661, 129597, 653503, 1178047,
    ),
    (3, 0): (
        2048, 274438, 798982, 4614, 16387, 32777, 14353, 51224, 291079, 801038, 1063310, 28807, 21006, 22550,
        569494, 1094038, 38930, 65566, 585886, 30753, 1110430, 55322, 292904, 1079567, 817193, 98327, 100503, 833815,
        78359, 602278, 63544, 117158, 1126559, 587810, 72095, 356398, 619039, 1143214, 110634, 88246, 897334, 102966,
        127027, 651454, 80318, 119358, 120999, 604583, 96807, 620719, 899631, 391599, 374839, 1161527, 915519, 1177919,
        3934080, 3934080, 3934080, 3934080, 3934080, 3934080, 3934080, 3934080, 3934080, 3934080, 3934080, 3934080, 3934080, 3934080,
        3934080, 3934080, 3934080, 3934080, 3934080, 3934080, 3934080, 3934080, 3934080, 3934080, 3934080, 3934080, 3934080, 3934080,
        3934080, 3934080, 3934080, 3934080, 3934080, 3934080, 3934080, 3934080, 3934080, 3934080, 3934080, 3934080,
    ),
    (3, 1): (
        2048, 270340, 794884, 1056774, 536710, 1061254, 4104, 18435, 34832, 272389, 534552, 14725, 1058841, 24711,
        286983, 549255, 811527, 1073166, 41102, 303374, 565646, 21006, 827414, 23060, 57494, 319766, 582038, 37398,
        843806, 39452, 323597, 289054, 550944, 67998, 1110413, 1075226, 30741, 55439, 555157, 567336, 1079701, 1091625,
        47503, 336023, 98340, 598295, 1122724, 833565, 321585, 584215, 78237, 340509, 602156, 864428, 63544, 326182,
        876844, 1138975, 849972, 630964, 117279, 356398, 1155508, 69934, 1143214, 372790, 634915, 123318, 385590, 909628,
        86588, 337957, 127269, 389541, 913451, 1124670, 79917, 354878, 102567, 878893, 604717, 1128871, 358447, 620595,
        370741, 895285, 883253, 119343, 120887, 125111, 649405, 1173949, 899383, 129591, 653503, 1178047,
    ),
}


def kernel(stages, micro_n, seq_n, model_n, hid_loc, heads_loc, head_dim,
           lens_ref, slopes_ref, x_hbm, wqkv_hbm, wout_hbm, wup_hbm, wdown_hbm,
           g1_ref, s1_ref, bqkv_ref, bo_ref, g2_ref, s2_ref, bup_ref, bd_ref,
           out_hbm,
           wqkv, wout, wup, wdown, xbuf, in1, in2, part, a_ref, u_ref, q_ref, kv_ref, ctx, ctxb, bq_ref,
           wq_sem, wo_sem, wu_sem, wd_sem, x_sem, in1_sem, in2_sem, s1_sem, s2_sem, f_sem, o_sem):
    tp = lax.axis_index('tp')
    pp = lax.axis_index('pp')
    nc = model_n // CH
    nw = model_n // WC
    nu = hid_loc // WC
    sub = WC // CH
    halves = seq_n // TOK
    units = micro_n * halves
    inner = (tp == 1) | (tp == 2)
    outer = (tp == 0) | (tp == 3)
    partner = tp + 1 - 2 * (tp % 2)
    peer = 3 - tp
    first = pp == 0
    later = pp > 0
    sends = pp < stages - 1

    def where(u):
        return lax.div(u, halves), pl.ds(pl.multiple_of(lax.rem(u, halves) * TOK, TOK), TOK)

    def x_copy(u, c):
        m, rows = where(u)
        return pltpu.make_async_copy(x_hbm.at[m, rows, pl.ds(c * CH, CH)], xbuf.at[u, c], x_sem.at[u, c])

    def wq_copy(c):
        return pltpu.make_async_copy(wqkv_hbm.at[c], wqkv.at[c], wq_sem.at[c])

    def wo_copy(c):
        return pltpu.make_async_copy(wout_hbm.at[:, pl.ds(c * WC, WC)], wout.at[c], wo_sem.at[c])

    def wu_copy(c):
        return pltpu.make_async_copy(wup_hbm.at[:, pl.ds(c * WC, WC)], wup.at[c], wu_sem.at[c])

    def wd_copy(c):
        return pltpu.make_async_copy(wdown_hbm.at[:, pl.ds(c * WC, WC)], wdown.at[c], wd_sem.at[c])

    @pl.when(first)
    def _():
        for c in range(nc):
            x_copy(jnp.int32(0), c).start()
    for c in range(3):
        wq_copy(c).start()
    for c in range(nw):
        wo_copy(c).start()
    for c in range(nu):
        wu_copy(c).start()
    for c in range(nw):
        wd_copy(c).start()

    @pl.when(first)
    def _():
        @pl.loop(1, units)
        def _(u):
            for c in range(nc):
                x_copy(u, c).start()

    barrier = pltpu.get_barrier_semaphore()
    links = ((tp > 0, {'tp': tp - 1}), (tp < 3, {'tp': tp + 1}), (later, {'pp': pp - 1}), (sends, {'pp': pp + 1}))
    for cond, dev in links:
        @pl.when(cond)
        def _(dev=dev):
            pl.semaphore_signal(barrier, inc=1, device_id=dev, device_id_type=MESH)
    mine = [(((pp == stage) & (inner if role else outer)).astype(jnp.int32), words) for (stage, role), words in TABLES.items()]
    table = [sum(sel * words[j] for sel, words in mine) for j in range(len(TABLES[0, 0]))]
    pl.semaphore_wait(barrier, sum(cond.astype(jnp.int32) for cond, _ in links))

    width = heads_loc * head_dim
    lane = lax.broadcasted_iota(jnp.int32, (head_dim, width), 1)
    row = lax.broadcasted_iota(jnp.int32, (head_dim, width), 0)
    pick = functools.reduce(jnp.logical_or, [lane == row + head_dim * h for h in range(heads_loc)])
    pick = pick.astype(jnp.float32).astype(jnp.bfloat16)
    low = lax.broadcasted_iota(jnp.int32, (heads_loc, width), 0) * head_dim
    lane = lax.broadcasted_iota(jnp.int32, (heads_loc, width), 1)
    own = (lane >= low) & (lane < low + head_dim)
    for c in range(3):
        spread = jnp.dot(bqkv_ref[0, c], pick, preferred_element_type=jnp.float32)
        bq_ref[c:c + 1, :] = jnp.sum(jnp.where(own, spread, 0.0), axis=0, keepdims=True)

    def part_copy(k, c):
        return pltpu.make_async_remote_copy(
            src_ref=part.at[k, c], dst_ref=in1.at[k, c], send_sem=s1_sem.at[k, c], recv_sem=in1_sem.at[k, c],
            device_id={'tp': partner}, device_id_type=MESH)

    def sum_copy(k, c):
        return pltpu.make_async_remote_copy(
            src_ref=part.at[k, c], dst_ref=in2.at[k, c], send_sem=s1_sem.at[k, c], recv_sem=in2_sem.at[k, c],
            device_id={'tp': peer}, device_id_type=MESH)

    def res_copy(k, c):
        return pltpu.make_async_remote_copy(
            src_ref=in1.at[k, c], dst_ref=in1.at[k, c], send_sem=s2_sem.at[k, c], recv_sem=in1_sem.at[k, c],
            device_id={'tp': partner}, device_id_type=MESH)

    def fwd_copy(u, c):
        return pltpu.make_async_remote_copy(
            src_ref=in1.at[2 * u + 1, c], dst_ref=xbuf.at[u, c], send_sem=f_sem.at[u, c], recv_sem=x_sem.at[u, c],
            device_id={'pp': pp + 1}, device_id_type=MESH)

    def out_copy(u, c):
        m, rows = where(u)
        return pltpu.make_async_copy(
            in1.at[2 * u + 1, c], out_hbm.at[m, rows, pl.ds(pl.multiple_of(c * CH, CH), CH)], o_sem.at[u, c])

    def cols(c, width=CH):
        return pl.ds(pl.multiple_of(c * width, width), width)

    rows_blk = 32

    def layer_norm(src, idx, gain, shift):
        @pl.loop(0, TOK // rows_blk)
        def _(r):
            rows = pl.ds(pl.multiple_of(r * rows_blk, rows_blk), rows_blk)
            val = jnp.concatenate([src[idx, c, rows, :] for c in range(nc)], axis=-1).astype(jnp.float32)
            mean = jnp.sum(val, axis=-1, keepdims=True) * (1.0 / model_n)
            cen = val - mean
            var = jnp.sum(cen * cen, axis=-1, keepdims=True) * (1.0 / model_n)
            normed = cen * lax.rsqrt(var + 1e-5)
            a_ref[rows, :] = (normed * gain[...].astype(jnp.float32) + shift[...].astype(jnp.float32)).astype(jnp.bfloat16)

    def attention(u):
        m = lax.div(u, halves)
        seq_len = lens_ref[m]
        qpos = lax.broadcasted_iota(jnp.int32, (TOK, seq_n), 0) + lax.rem(u, halves) * TOK
        kpos = lax.broadcasted_iota(jnp.int32, (TOK, seq_n), 1)
        allowed = (kpos <= qpos) & (kpos < seq_len)
        dist = (qpos - kpos).astype(jnp.float32)
        ctx[...] = jnp.zeros_like(ctx)

        @pl.loop(0, heads_loc // 2)
        def _(g):
            win = pl.ds(pl.multiple_of(g * 128, 128), 256)
            lane = lax.broadcasted_iota(jnp.int32, (1, 256), 1) + g * 128
            low = 2 * head_dim * g
            m0 = ((lane >= low) & (lane < low + head_dim)).astype(jnp.float32).astype(jnp.bfloat16)
            m1 = ((lane >= low + head_dim) & (lane < low + 2 * head_dim)).astype(jnp.float32).astype(jnp.bfloat16)
            key = kv_ref[0, :, win]
            val = kv_ref[1, :, win]
            kk = jnp.concatenate([key * m0, key * m1], axis=0)
            vv = jnp.concatenate([val * m0, val * m1], axis=0)
            sc = lax.dot_general(q_ref[:, win], kk, (((1,), (1,)), ((), ())), preferred_element_type=jnp.float32)
            probs = []
            for j in range(2):
                s = sc[:, j * seq_n:(j + 1) * seq_n] * (head_dim ** -0.5)
                s = s - slopes_ref[tp * heads_loc + 2 * g + j] * dist
                s = jnp.where(allowed, s, -1e30)
                e = jnp.exp(s - jnp.max(s, axis=-1, keepdims=True))
                probs.append((e / jnp.sum(e, axis=-1, keepdims=True)).astype(jnp.bfloat16))
            o = jnp.dot(jnp.concatenate(probs, axis=-1), vv, preferred_element_type=jnp.float32)
            ctx[:, win] += o
        ctxb[...] = ctx[...].astype(jnp.bfloat16)

    def own_partial(u, a, lhs, w, w_copy):
        k = 2 * u + a

        @pl.loop(0, nw)
        def _(w_idx):
            @pl.when(u == 0)
            def _():
                w_copy(w_idx).wait()
            val = jnp.dot(lhs[...], w[w_idx], preferred_element_type=jnp.float32).astype(jnp.bfloat16)
            for j in range(sub):
                part[k, w_idx * sub + j] = val[:, j * CH:(j + 1) * CH]

            @pl.when(outer)
            def _():
                for j in range(sub):
                    part_copy(k, w_idx * sub + j).start()

    def p1a(u):
        _, rows = where(u)
        for c in range(nc):
            x_copy(u, c).wait()
        layer_norm(xbuf, u, g1_ref, s1_ref)
        if halves > 1:
            @pl.when(lax.rem(u, halves) == 0)
            def _():
                kv_ref[:, TOK:, :] = jnp.zeros((2, seq_n - TOK, kv_ref.shape[2]), kv_ref.dtype)
        for c in range(3):
            @pl.when(u == 0)
            def _(c=c):
                wq_copy(c).wait()
            acc = jnp.dot(a_ref[...], wqkv[c], preferred_element_type=jnp.float32)
            acc = (acc + bq_ref[c:c + 1, :]).astype(jnp.bfloat16)
            if c == 0:
                q_ref[...] = acc
            else:
                kv_ref[c - 1, rows, :] = acc

    def p1b(u):
        attention(u)
        own_partial(u, 0, ctxb, wout, wo_copy)

    def p2a(u):
        layer_norm(in1, 2 * u, g2_ref, s2_ref)

        @pl.loop(0, nu)
        def _(c):
            @pl.when(u == 0)
            def _():
                wu_copy(c).wait()
            t = jnp.dot(a_ref[...], wup[c], preferred_element_type=jnp.float32) + bup_ref[:, cols(c, WC)].astype(jnp.float32)
            t = 0.5 * t * (1.0 + jnp.tanh(math.sqrt(2.0 / math.pi) * (t + 0.044715 * (t * t * t))))
            u_ref[:, cols(c, WC)] = t.astype(jnp.bfloat16)

    def p2b(u):
        own_partial(u, 1, u_ref, wdown, wd_copy)

    def r1(u, a, c):
        k = 2 * u + a
        part_copy(k, c).wait_recv()
        part[k, c] = (part[k, c].astype(jnp.float32) + in1[k, c].astype(jnp.float32)).astype(jnp.bfloat16)
        sum_copy(k, c).start()

    def r2(u, a, c):
        k = 2 * u + a
        bias = bo_ref if a == 0 else bd_ref

        @pl.when(inner)
        def _():
            sum_copy(k, c).wait_recv()
            resid = xbuf[u, c] if a == 0 else in1[2 * u, c]
            total = part[k, c].astype(jnp.float32) + in2[k, c].astype(jnp.float32)
            in1[k, c] = (resid.astype(jnp.float32) + total + bias[:, cols(c)].astype(jnp.float32)).astype(jnp.bfloat16)
            res_copy(k, c).start()

        @pl.when(outer)
        def _():
            part_copy(k, c).wait_recv()
        if a == 1:
            @pl.when(sends)
            def _():
                fwd_copy(u, c).start()
            out_copy(u, c).start()

    ops = (p1a, p1b, p2a, p2b)

    def step(_, word):
        entry = lax.rem(word, 2048)
        op, u, c = lax.rem(entry, 8), lax.rem(lax.div(entry, 8), 16), lax.div(entry, 128)

        @pl.when(op < 4)
        def _():
            for i, fn in enumerate(ops):
                @pl.when((op == i) & (c == 0))
                def _(fn=fn):
                    fn(u)

        @pl.when(op >= 4)
        def _():
            for a in range(2):
                @pl.when(op == 4 + a)
                def _(a=a):
                    r1(u, a, c)

                @pl.when(op == 6 + a)
                def _(a=a):
                    r2(u, a, c)
        return lax.div(word, 2048)

    def two_steps(_, group):
        lax.fori_loop(0, 2, step, group[0])
        return group[1:] + group[:1]

    @pl.loop(0, len(table) // 8)
    def _(t):
        hits = [(t == i).astype(jnp.int32) for i in range(len(table) // 8)]
        group = tuple(sum(hit * table[8 * i + j] for i, hit in enumerate(hits)) for j in range(8))
        lax.fori_loop(0, 8, two_steps, group)

    @pl.loop(0, 2 * units)
    def _(k):
        for c in range(nc):
            part_copy(k, c).wait_send()

        @pl.when(inner)
        def _():
            for c in range(nc):
                res_copy(k, c).wait_send()

    @pl.loop(0, units)
    def _(u):
        @pl.when(sends)
        def _():
            for c in range(nc):
                fwd_copy(u, c).wait_send()
        for c in range(nc):
            out_copy(u, c).wait()


def solution(mesh):
    stages = mesh.shape['pp']
    in_specs = (P('dp'), P('dp'), P('pp'), P('pp'), P('pp', None, None, 'tp'), P('pp', None, 'tp', None), P('pp', 'tp', None), P('pp'), P('pp'), P('pp'), P('pp', None, 'tp'), P('pp', 'tp'), P('pp', 'tp', None), P('pp'))

    def per_device(x_in, seq_lens, ln1_gain, ln1_shift, w_qkv, b_qkv, w_out, b_out, ln2_gain, ln2_shift, w_up, b_up, w_down, b_down):
        micro_n, batch_n, seq_n, model_n = x_in.shape
        heads_loc, head_dim = b_qkv.shape[2], b_qkv.shape[3]
        width_loc = heads_loc * head_dim
        hid_loc = w_up.shape[2]
        nc, nw, nu = model_n // CH, model_n // WC, hid_loc // WC
        units = micro_n * seq_n // TOK
        assert batch_n == 1 and mesh.shape['tp'] == 4 and seq_n == 128
        slopes = alibi_slopes(heads_loc * mesh.shape['tp'])
        bf = jnp.bfloat16
        vm = pl.BlockSpec(memory_space=pltpu.VMEM)
        sm = pl.BlockSpec(memory_space=pltpu.SMEM)
        hb = pl.BlockSpec(memory_space=pl.ANY)
        dma = pltpu.SemaphoreType.DMA
        body = functools.partial(kernel, stages, micro_n, seq_n, model_n, hid_loc, heads_loc, head_dim)
        out = pl.pallas_call(
            body,
            out_shape=jax.ShapeDtypeStruct((micro_n, seq_n, model_n), bf),
            in_specs=[sm, sm] + [hb] * 5 + [vm] * 8,
            out_specs=hb,
            scratch_shapes=[
                pltpu.VMEM((3, model_n, width_loc), bf),
                pltpu.VMEM((nw, width_loc, WC), bf),
                pltpu.VMEM((nu, model_n, WC), bf),
                pltpu.VMEM((nw, hid_loc, WC), bf),
                pltpu.VMEM((units, nc, TOK, CH), bf),
                pltpu.VMEM((2 * units, nc, TOK, CH), bf),
                pltpu.VMEM((2 * units, nc, TOK, CH), bf),
                pltpu.VMEM((2 * units, nc, TOK, CH), bf),
                pltpu.VMEM((TOK, model_n), bf),
                pltpu.VMEM((TOK, hid_loc), bf),
                pltpu.VMEM((TOK, width_loc), bf),
                pltpu.VMEM((2, seq_n, width_loc), bf),
                pltpu.VMEM((TOK, width_loc), jnp.float32),
                pltpu.VMEM((TOK, width_loc), bf),
                pltpu.VMEM((3, width_loc), jnp.float32),
                dma((3,)), dma((nw,)), dma((nu,)), dma((nw,)),
                dma((units, nc)), dma((2 * units, nc)), dma((2 * units, nc)),
                dma((2 * units, nc)), dma((2 * units, nc)), dma((units, nc)), dma((units, nc)),
            ],
            compiler_params=pltpu.CompilerParams(
                collective_id=0, has_side_effects=True, vmem_limit_bytes=67043328),
            name='stages',
        )(
            seq_lens.reshape(micro_n), slopes,
            x_in.reshape(micro_n, seq_n, model_n),
            jnp.transpose(w_qkv[0], (1, 0, 2)), w_out[0], w_up[0], w_down[0],
            ln1_gain, ln1_shift, b_qkv, b_out, ln2_gain, ln2_shift, b_up, b_down,
        )
        return out.reshape(1, micro_n, batch_n, seq_n, model_n)

    return jax.shard_map(per_device, mesh=mesh, in_specs=in_specs, out_specs=P('pp', 'dp'), check_vma=False)
```

```python
import functools
import math

import jax
import jax.numpy as jnp
from jax import lax
from jax.experimental import pallas as pl
from jax.experimental.pallas import tpu as pltpu
from jax.sharding import PartitionSpec as P

MESH = pl.DeviceIdType.MESH
CH = 256
WC = 512


def alibi_slopes(heads_n):
    closest = 2 ** int(math.floor(math.log2(heads_n)))
    base_rate = 2.0 ** (-8.0 / closest)
    slope_list = [base_rate ** (head_idx + 1) for head_idx in range(closest)]
    extra_rate = 2.0 ** (-4.0 / closest)
    slope_list = slope_list + [extra_rate ** (2 * head_idx + 1) for head_idx in range(min(closest, heads_n - closest))]
    return jnp.array(slope_list, dtype=jnp.float32)


def kernel(stages, micro_n, seq_n, model_n, hid_loc, heads_loc, head_dim,
           lens_ref, slopes_ref, x_hbm, wqkv_hbm, wout_hbm, wup_hbm, wdown_hbm,
           g1_ref, s1_ref, bqkv_ref, bo_ref, g2_ref, s2_ref, bup_ref, bd_ref,
           out_hbm,
           wqkv, wout, wup, wdown, xbuf, in1, in2, part, a_ref, u_ref, qkv, ctx, ctxb, bq_ref,
           wq_sem, wo_sem, wu_sem, wd_sem, x_sem, in1_sem, in2_sem, s1_sem, s2_sem, f_sem, o_sem):
    tp = lax.axis_index('tp')
    pp = lax.axis_index('pp')
    nc = model_n // CH
    nw = model_n // WC
    nu = hid_loc // WC
    sub = WC // CH
    inner = (tp == 1) | (tp == 2)
    outer = (tp == 0) | (tp == 3)
    partner = tp + 1 - 2 * (tp % 2)
    peer = 3 - tp
    first = pp == 0
    later = pp > 0
    sends = pp < stages - 1

    def x_copy(u, c):
        return pltpu.make_async_copy(x_hbm.at[u, :, pl.ds(c * CH, CH)], xbuf.at[u, c], x_sem.at[u, c])

    def wq_copy(c):
        return pltpu.make_async_copy(wqkv_hbm.at[c], wqkv.at[c], wq_sem.at[c])

    def wo_copy(c):
        return pltpu.make_async_copy(wout_hbm.at[:, pl.ds(c * WC, WC)], wout.at[c], wo_sem.at[c])

    def wu_copy(c):
        return pltpu.make_async_copy(wup_hbm.at[:, pl.ds(c * WC, WC)], wup.at[c], wu_sem.at[c])

    def wd_copy(c):
        return pltpu.make_async_copy(wdown_hbm.at[:, pl.ds(c * WC, WC)], wdown.at[c], wd_sem.at[c])

    @pl.when(first)
    def _():
        for c in range(nc):
            x_copy(0, c).start()
    for c in range(3):
        wq_copy(c).start()
    for c in range(nw):
        wo_copy(c).start()
    for c in range(nu):
        wu_copy(c).start()
    for c in range(nw):
        wd_copy(c).start()

    @pl.when(first)
    def _():
        for u in range(1, micro_n):
            for c in range(nc):
                x_copy(u, c).start()

    barrier = pltpu.get_barrier_semaphore()
    links = ((tp > 0, {'tp': tp - 1}), (tp < 3, {'tp': tp + 1}), (later, {'pp': pp - 1}), (sends, {'pp': pp + 1}))
    for cond, dev in links:
        @pl.when(cond)
        def _(dev=dev):
            pl.semaphore_signal(barrier, inc=1, device_id=dev, device_id_type=MESH)
    pl.semaphore_wait(barrier, sum(cond.astype(jnp.int32) for cond, _ in links))

    width = heads_loc * head_dim
    lane = lax.broadcasted_iota(jnp.int32, (head_dim, width), 1)
    row = lax.broadcasted_iota(jnp.int32, (head_dim, width), 0)
    pick = functools.reduce(jnp.logical_or, [lane == row + head_dim * h for h in range(heads_loc)])
    pick = pick.astype(jnp.float32).astype(jnp.bfloat16)
    low = lax.broadcasted_iota(jnp.int32, (heads_loc, width), 0) * head_dim
    lane = lax.broadcasted_iota(jnp.int32, (heads_loc, width), 1)
    own = (lane >= low) & (lane < low + head_dim)
    for c in range(3):
        spread = jnp.dot(bqkv_ref[0, c], pick, preferred_element_type=jnp.float32)
        bq_ref[c:c + 1, :] = jnp.sum(jnp.where(own, spread, 0.0), axis=0, keepdims=True)

    def part_copy(k, c):
        return pltpu.make_async_remote_copy(
            src_ref=part.at[k % 2, c], dst_ref=in1.at[k, c], send_sem=s1_sem.at[k, c], recv_sem=in1_sem.at[k, c],
            device_id={'tp': partner}, device_id_type=MESH)

    def sum_copy(k, c):
        return pltpu.make_async_remote_copy(
            src_ref=part.at[k % 2, c], dst_ref=in2.at[k, c], send_sem=s1_sem.at[k, c], recv_sem=in2_sem.at[k, c],
            device_id={'tp': peer}, device_id_type=MESH)

    def res_copy(k, c):
        return pltpu.make_async_remote_copy(
            src_ref=in1.at[k, c], dst_ref=in1.at[k, c], send_sem=s2_sem.at[k, c], recv_sem=in1_sem.at[k, c],
            device_id={'tp': partner}, device_id_type=MESH)

    def fwd_copy(u, c):
        return pltpu.make_async_remote_copy(
            src_ref=in1.at[2 * u + 1, c], dst_ref=xbuf.at[u, c], send_sem=f_sem.at[u, c], recv_sem=x_sem.at[u, c],
            device_id={'pp': pp + 1}, device_id_type=MESH)

    def out_copy(u, c):
        return pltpu.make_async_copy(in1.at[2 * u + 1, c], out_hbm.at[u, :, pl.ds(c * CH, CH)], o_sem.at[u, c])

    def cols(c, width=CH):
        return pl.ds(pl.multiple_of(c * width, width), width)

    rows_blk = 32

    def layer_norm(src, idx, gain, shift):
        @pl.loop(0, seq_n // rows_blk)
        def _(r):
            rows = pl.ds(pl.multiple_of(r * rows_blk, rows_blk), rows_blk)
            val = jnp.concatenate([src[idx, c, rows, :] for c in range(nc)], axis=-1).astype(jnp.float32)
            mean = jnp.sum(val, axis=-1, keepdims=True) * (1.0 / model_n)
            cen = val - mean
            var = jnp.sum(cen * cen, axis=-1, keepdims=True) * (1.0 / model_n)
            normed = cen * lax.rsqrt(var + 1e-5)
            a_ref[rows, :] = (normed * gain[...].astype(jnp.float32) + shift[...].astype(jnp.float32)).astype(jnp.bfloat16)

    def attention(u):
        seq_len = lens_ref[u]
        qpos = lax.broadcasted_iota(jnp.int32, (seq_n, seq_n), 0)
        kpos = lax.broadcasted_iota(jnp.int32, (seq_n, seq_n), 1)
        allowed = (kpos <= qpos) & (kpos < seq_len)
        dist = (qpos - kpos).astype(jnp.float32)
        ctx[...] = jnp.zeros_like(ctx)

        @pl.loop(0, heads_loc // 2)
        def _(g):
            win = pl.ds(pl.multiple_of(g * 128, 128), 256)
            lane = lax.broadcasted_iota(jnp.int32, (1, 256), 1) + g * 128
            low = 2 * head_dim * g
            m0 = ((lane >= low) & (lane < low + head_dim)).astype(jnp.float32).astype(jnp.bfloat16)
            m1 = ((lane >= low + head_dim) & (lane < low + 2 * head_dim)).astype(jnp.float32).astype(jnp.bfloat16)
            key = qkv[1, :, win]
            val = qkv[2, :, win]
            kk = jnp.concatenate([key * m0, key * m1], axis=0)
            vv = jnp.concatenate([val * m0, val * m1], axis=0)
            sc = lax.dot_general(qkv[0, :, win], kk, (((1,), (1,)), ((), ())), preferred_element_type=jnp.float32)
            probs = []
            for j in range(2):
                s = sc[:, j * seq_n:(j + 1) * seq_n] * (head_dim ** -0.5)
                s = s - slopes_ref[tp * heads_loc + 2 * g + j] * dist
                s = jnp.where(allowed, s, -1e30)
                e = jnp.exp(s - jnp.max(s, axis=-1, keepdims=True))
                probs.append((e / jnp.sum(e, axis=-1, keepdims=True)).astype(jnp.bfloat16))
            o = jnp.dot(jnp.concatenate(probs, axis=-1), vv, preferred_element_type=jnp.float32)
            ctx[:, win] += o
        ctxb[...] = ctx[...].astype(jnp.bfloat16)

    def own_partial(s, a, lhs, w, w_copy):
        k = 2 * s + a

        @pl.loop(0, nw)
        def _(w_idx):
            @pl.when(s == 0)
            def _():
                w_copy(w_idx).wait()

            @pl.when(s > 0)
            def _():
                for j in range(sub):
                    part_copy(k - 2, w_idx * sub + j).wait_send()
            val = jnp.dot(lhs[...], w[w_idx], preferred_element_type=jnp.float32).astype(jnp.bfloat16)
            for j in range(sub):
                part[a, w_idx * sub + j] = val[:, j * CH:(j + 1) * CH]

            @pl.when(outer)
            def _():
                for j in range(sub):
                    part_copy(k, w_idx * sub + j).start()

    def p1(s):
        for c in range(nc):
            x_copy(s, c).wait()
        layer_norm(xbuf, s, g1_ref, s1_ref)

        for c in range(3):
            @pl.when(s == 0)
            def _(c=c):
                wq_copy(c).wait()
            acc = jnp.dot(a_ref[...], wqkv[c], preferred_element_type=jnp.float32)
            qkv[c] = (acc + bq_ref[c:c + 1, :]).astype(jnp.bfloat16)
        attention(s)
        own_partial(s, 0, ctxb, wout, wo_copy)

    def p2(s):
        layer_norm(in1, 2 * s, g2_ref, s2_ref)

        @pl.loop(0, nu)
        def _(c):
            @pl.when(s == 0)
            def _():
                wu_copy(c).wait()
            t = jnp.dot(a_ref[...], wup[c], preferred_element_type=jnp.float32) + bup_ref[:, cols(c, WC)].astype(jnp.float32)
            t = 0.5 * t * (1.0 + jnp.tanh(math.sqrt(2.0 / math.pi) * (t + 0.044715 * (t * t * t))))
            u_ref[:, cols(c, WC)] = t.astype(jnp.bfloat16)
        own_partial(s, 1, u_ref, wdown, wd_copy)

    lag = 6

    def reduce(s, a):
        k = 2 * s + a
        bias = bo_ref if a == 0 else bd_ref

        def forward(c):
            part_copy(k, c).wait_recv()
            part[a, c] = (part[a, c].astype(jnp.float32) + in1[k, c].astype(jnp.float32)).astype(jnp.bfloat16)
            sum_copy(k, c).start()

        def leave(c):
            if a == 1:
                @pl.when(sends)
                def _():
                    fwd_copy(s, c).start()
                out_copy(s, c).start()

        def finish(c):
            sum_copy(k, c).wait_recv()
            resid = xbuf[s, c] if a == 0 else in1[2 * s, c]
            total = part[a, c].astype(jnp.float32) + in2[k, c].astype(jnp.float32)
            in1[k, c] = (resid.astype(jnp.float32) + total + bias[:, cols(c)].astype(jnp.float32)).astype(jnp.bfloat16)
            res_copy(k, c).start()
            leave(c)

        @pl.when(inner)
        def _():
            @pl.loop(0, nc + lag)
            def _(i):
                @pl.when(i < nc)
                def _():
                    forward(i)

                @pl.when(i >= lag)
                def _():
                    finish(i - lag)

        @pl.when(outer)
        def _():
            @pl.loop(0, nc)
            def _(c):
                part_copy(k, c).wait_recv()
                leave(c)

    @pl.loop(0, micro_n + 1)
    def _(s):
        @pl.when(s < micro_n)
        def _():
            p1(s)

        @pl.when(s > 0)
        def _():
            reduce(s - 1, 1)

        @pl.when(s < micro_n)
        def _():
            reduce(s, 0)
            p2(s)

    last = micro_n - 1
    for a in range(2):
        for c in range(nc):
            part_copy(2 * last + a, c).wait_send()

    @pl.when(inner)
    def _():
        @pl.loop(0, 2 * micro_n)
        def _(k):
            @pl.loop(0, nc)
            def _(c):
                res_copy(k, c).wait_send()

    @pl.loop(0, micro_n)
    def _(u):
        @pl.loop(0, nc)
        def _(c):
            @pl.when(sends)
            def _():
                fwd_copy(u, c).wait_send()
            out_copy(u, c).wait()


def solution(mesh):
    stages = mesh.shape['pp']
    in_specs = (P('dp'), P('dp'), P('pp'), P('pp'), P('pp', None, None, 'tp'), P('pp', None, 'tp', None), P('pp', 'tp', None), P('pp'), P('pp'), P('pp'), P('pp', None, 'tp'), P('pp', 'tp'), P('pp', 'tp', None), P('pp'))

    def per_device(x_in, seq_lens, ln1_gain, ln1_shift, w_qkv, b_qkv, w_out, b_out, ln2_gain, ln2_shift, w_up, b_up, w_down, b_down):
        micro_n, batch_n, seq_n, model_n = x_in.shape
        heads_loc, head_dim = b_qkv.shape[2], b_qkv.shape[3]
        width_loc = heads_loc * head_dim
        hid_loc = w_up.shape[2]
        nc, nw, nu = model_n // CH, model_n // WC, hid_loc // WC
        assert batch_n == 1 and mesh.shape['tp'] == 4 and seq_n == 128
        slopes = alibi_slopes(heads_loc * mesh.shape['tp'])
        bf = jnp.bfloat16
        vm = pl.BlockSpec(memory_space=pltpu.VMEM)
        sm = pl.BlockSpec(memory_space=pltpu.SMEM)
        hb = pl.BlockSpec(memory_space=pl.ANY)
        dma = pltpu.SemaphoreType.DMA
        body = functools.partial(kernel, stages, micro_n, seq_n, model_n, hid_loc, heads_loc, head_dim)
        out = pl.pallas_call(
            body,
            out_shape=jax.ShapeDtypeStruct((micro_n, seq_n, model_n), bf),
            in_specs=[sm, sm] + [hb] * 5 + [vm] * 8,
            out_specs=hb,
            scratch_shapes=[
                pltpu.VMEM((3, model_n, width_loc), bf),
                pltpu.VMEM((nw, width_loc, WC), bf),
                pltpu.VMEM((nu, model_n, WC), bf),
                pltpu.VMEM((nw, hid_loc, WC), bf),
                pltpu.VMEM((micro_n, nc, seq_n, CH), bf),
                pltpu.VMEM((2 * micro_n, nc, seq_n, CH), bf),
                pltpu.VMEM((2 * micro_n, nc, seq_n, CH), bf),
                pltpu.VMEM((2, nc, seq_n, CH), bf),
                pltpu.VMEM((seq_n, model_n), bf),
                pltpu.VMEM((seq_n, hid_loc), bf),
                pltpu.VMEM((3, seq_n, width_loc), bf),
                pltpu.VMEM((seq_n, width_loc), jnp.float32),
                pltpu.VMEM((seq_n, width_loc), bf),
                pltpu.VMEM((3, width_loc), jnp.float32),
                dma((3,)), dma((nw,)), dma((nu,)), dma((nw,)),
                dma((micro_n, nc)), dma((2 * micro_n, nc)), dma((2 * micro_n, nc)),
                dma((2 * micro_n, nc)), dma((2 * micro_n, nc)), dma((micro_n, nc)), dma((micro_n, nc)),
            ],
            compiler_params=pltpu.CompilerParams(
                collective_id=0, has_side_effects=True, vmem_limit_bytes=67043328),
            name='stages',
        )(
            seq_lens.reshape(micro_n), slopes,
            x_in.reshape(micro_n, seq_n, model_n),
            jnp.transpose(w_qkv[0], (1, 0, 2)), w_out[0], w_up[0], w_down[0],
            ln1_gain, ln1_shift, b_qkv, b_out, ln2_gain, ln2_shift, b_up, b_down,
        )
        return out.reshape(1, micro_n, batch_n, seq_n, model_n)

    return jax.shard_map(per_device, mesh=mesh, in_specs=in_specs, out_specs=P('pp', 'dp'), check_vma=False)
```

```python
import functools
import math

import jax
import jax.numpy as jnp
from jax import lax
from jax.experimental import pallas as pl
from jax.experimental.pallas import tpu as pltpu
from jax.sharding import PartitionSpec as P

MESH = pl.DeviceIdType.MESH
CH = 256
WC = 512


def alibi_slopes(heads_n):
    closest = 2 ** int(math.floor(math.log2(heads_n)))
    base_rate = 2.0 ** (-8.0 / closest)
    slope_list = [base_rate ** (head_idx + 1) for head_idx in range(closest)]
    extra_rate = 2.0 ** (-4.0 / closest)
    slope_list = slope_list + [extra_rate ** (2 * head_idx + 1) for head_idx in range(min(closest, heads_n - closest))]
    return jnp.array(slope_list, dtype=jnp.float32)


def kernel(stages, micro_n, seq_n, model_n, hid_loc, heads_loc, head_dim,
           lens_ref, slopes_ref, x_hbm, wqkv_hbm, wout_hbm, wup_hbm, wdown_hbm,
           g1_ref, s1_ref, bqkv_ref, bo_ref, g2_ref, s2_ref, bup_ref, bd_ref,
           out_hbm,
           wqkv, wout, wup, wdown, xbuf, in1, in2, part, a_ref, u_ref, qkv, ctx, ctxb, bq_ref,
           wq_sem, wo_sem, wu_sem, wd_sem, x_sem, in1_sem, in2_sem, s1_sem, s2_sem, f_sem, o_sem):
    tp = lax.axis_index('tp')
    pp = lax.axis_index('pp')
    nc = model_n // CH
    nw = model_n // WC
    nu = hid_loc // WC
    sub = WC // CH
    inner = (tp == 1) | (tp == 2)
    outer = (tp == 0) | (tp == 3)
    partner = tp + 1 - 2 * (tp % 2)
    peer = 3 - tp
    first = pp == 0
    later = pp > 0
    sends = pp < stages - 1

    def x_copy(u, c):
        return pltpu.make_async_copy(x_hbm.at[u, :, pl.ds(c * CH, CH)], xbuf.at[u, c], x_sem.at[u, c])

    def wq_copy(c):
        return pltpu.make_async_copy(wqkv_hbm.at[c], wqkv.at[c], wq_sem.at[c])

    def wo_copy(c):
        return pltpu.make_async_copy(wout_hbm.at[:, pl.ds(c * WC, WC)], wout.at[c], wo_sem.at[c])

    def wu_copy(c):
        return pltpu.make_async_copy(wup_hbm.at[:, pl.ds(c * WC, WC)], wup.at[c], wu_sem.at[c])

    def wd_copy(c):
        return pltpu.make_async_copy(wdown_hbm.at[:, pl.ds(c * WC, WC)], wdown.at[c], wd_sem.at[c])

    @pl.when(first)
    def _():
        for c in range(nc):
            x_copy(0, c).start()
    for c in range(3):
        wq_copy(c).start()
    for c in range(nw):
        wo_copy(c).start()
    for c in range(nu):
        wu_copy(c).start()
    for c in range(nw):
        wd_copy(c).start()

    @pl.when(first)
    def _():
        for u in range(1, micro_n):
            for c in range(nc):
                x_copy(u, c).start()

    barrier = pltpu.get_barrier_semaphore()
    links = ((tp > 0, {'tp': tp - 1}), (tp < 3, {'tp': tp + 1}), (later, {'pp': pp - 1}), (sends, {'pp': pp + 1}))
    for cond, dev in links:
        @pl.when(cond)
        def _(dev=dev):
            pl.semaphore_signal(barrier, inc=1, device_id=dev, device_id_type=MESH)
    pl.semaphore_wait(barrier, sum(cond.astype(jnp.int32) for cond, _ in links))

    width = heads_loc * head_dim
    lane = lax.broadcasted_iota(jnp.int32, (head_dim, width), 1)
    row = lax.broadcasted_iota(jnp.int32, (head_dim, width), 0)
    pick = functools.reduce(jnp.logical_or, [lane == row + head_dim * h for h in range(heads_loc)])
    pick = pick.astype(jnp.float32).astype(jnp.bfloat16)
    low = lax.broadcasted_iota(jnp.int32, (heads_loc, width), 0) * head_dim
    lane = lax.broadcasted_iota(jnp.int32, (heads_loc, width), 1)
    own = (lane >= low) & (lane < low + head_dim)
    for c in range(3):
        spread = jnp.dot(bqkv_ref[0, c], pick, preferred_element_type=jnp.float32)
        bq_ref[c:c + 1, :] = jnp.sum(jnp.where(own, spread, 0.0), axis=0, keepdims=True)

    def part_copy(k, c):
        return pltpu.make_async_remote_copy(
            src_ref=part.at[k % 2, c], dst_ref=in1.at[k, c], send_sem=s1_sem.at[k, c], recv_sem=in1_sem.at[k, c],
            device_id={'tp': partner}, device_id_type=MESH)

    def sum_copy(k, c):
        return pltpu.make_async_remote_copy(
            src_ref=part.at[k % 2, c], dst_ref=in2.at[k, c], send_sem=s1_sem.at[k, c], recv_sem=in2_sem.at[k, c],
            device_id={'tp': peer}, device_id_type=MESH)

    def res_copy(k, c):
        return pltpu.make_async_remote_copy(
            src_ref=in1.at[k, c], dst_ref=in1.at[k, c], send_sem=s2_sem.at[k, c], recv_sem=in1_sem.at[k, c],
            device_id={'tp': partner}, device_id_type=MESH)

    def fwd_copy(u, c):
        return pltpu.make_async_remote_copy(
            src_ref=in1.at[2 * u + 1, c], dst_ref=xbuf.at[u, c], send_sem=f_sem.at[u, c], recv_sem=x_sem.at[u, c],
            device_id={'pp': pp + 1}, device_id_type=MESH)

    def out_copy(u, c):
        return pltpu.make_async_copy(in1.at[2 * u + 1, c], out_hbm.at[u, :, pl.ds(c * CH, CH)], o_sem.at[u, c])

    def cols(c, width=CH):
        return pl.ds(pl.multiple_of(c * width, width), width)

    rows_blk = 32

    def layer_norm(src, idx, gain, shift):
        @pl.loop(0, seq_n // rows_blk)
        def _(r):
            rows = pl.ds(pl.multiple_of(r * rows_blk, rows_blk), rows_blk)
            val = jnp.concatenate([src[idx, c, rows, :] for c in range(nc)], axis=-1).astype(jnp.float32)
            mean = jnp.sum(val, axis=-1, keepdims=True) * (1.0 / model_n)
            cen = val - mean
            var = jnp.sum(cen * cen, axis=-1, keepdims=True) * (1.0 / model_n)
            normed = cen * lax.rsqrt(var + 1e-5)
            a_ref[rows, :] = (normed * gain[...].astype(jnp.float32) + shift[...].astype(jnp.float32)).astype(jnp.bfloat16)

    def attention(u):
        seq_len = lens_ref[u]
        qpos = lax.broadcasted_iota(jnp.int32, (seq_n, seq_n), 0)
        kpos = lax.broadcasted_iota(jnp.int32, (seq_n, seq_n), 1)
        allowed = (kpos <= qpos) & (kpos < seq_len)
        dist = (qpos - kpos).astype(jnp.float32)
        ctx[...] = jnp.zeros_like(ctx)

        @pl.loop(0, heads_loc // 2)
        def _(g):
            win = pl.ds(pl.multiple_of(g * 128, 128), 256)
            lane = lax.broadcasted_iota(jnp.int32, (1, 256), 1) + g * 128
            low = 2 * head_dim * g
            m0 = ((lane >= low) & (lane < low + head_dim)).astype(jnp.float32).astype(jnp.bfloat16)
            m1 = ((lane >= low + head_dim) & (lane < low + 2 * head_dim)).astype(jnp.float32).astype(jnp.bfloat16)
            key = qkv[1, :, win]
            val = qkv[2, :, win]
            kk = jnp.concatenate([key * m0, key * m1], axis=0)
            vv = jnp.concatenate([val * m0, val * m1], axis=0)
            sc = lax.dot_general(qkv[0, :, win], kk, (((1,), (1,)), ((), ())), preferred_element_type=jnp.float32)
            probs = []
            for j in range(2):
                s = sc[:, j * seq_n:(j + 1) * seq_n] * (head_dim ** -0.5)
                s = s - slopes_ref[tp * heads_loc + 2 * g + j] * dist
                s = jnp.where(allowed, s, -1e30)
                e = jnp.exp(s - jnp.max(s, axis=-1, keepdims=True))
                probs.append((e / jnp.sum(e, axis=-1, keepdims=True)).astype(jnp.bfloat16))
            o = jnp.dot(jnp.concatenate(probs, axis=-1), vv, preferred_element_type=jnp.float32)
            ctx[:, win] += o
        ctxb[...] = ctx[...].astype(jnp.bfloat16)

    def own_partial(s, a, lhs, w, w_copy):
        k = 2 * s + a

        @pl.loop(0, nw)
        def _(w_idx):
            @pl.when(s == 0)
            def _():
                w_copy(w_idx).wait()

            @pl.when(s > 0)
            def _():
                for j in range(sub):
                    part_copy(k - 2, w_idx * sub + j).wait_send()
            val = jnp.dot(lhs[...], w[w_idx], preferred_element_type=jnp.float32).astype(jnp.bfloat16)
            for j in range(sub):
                part[a, w_idx * sub + j] = val[:, j * CH:(j + 1) * CH]

            @pl.when(outer)
            def _():
                for j in range(sub):
                    part_copy(k, w_idx * sub + j).start()

    def p1(s):
        for c in range(nc):
            x_copy(s, c).wait()
        layer_norm(xbuf, s, g1_ref, s1_ref)

        for c in range(3):
            @pl.when(s == 0)
            def _(c=c):
                wq_copy(c).wait()
            acc = jnp.dot(a_ref[...], wqkv[c], preferred_element_type=jnp.float32)
            qkv[c] = (acc + bq_ref[c:c + 1, :]).astype(jnp.bfloat16)
        attention(s)
        own_partial(s, 0, ctxb, wout, wo_copy)

    def p2(s):
        layer_norm(in1, 2 * s, g2_ref, s2_ref)

        @pl.loop(0, nu)
        def _(c):
            @pl.when(s == 0)
            def _():
                wu_copy(c).wait()
            t = jnp.dot(a_ref[...], wup[c], preferred_element_type=jnp.float32) + bup_ref[:, cols(c, WC)].astype(jnp.float32)
            t = 0.5 * t * (1.0 + jnp.tanh(math.sqrt(2.0 / math.pi) * (t + 0.044715 * (t * t * t))))
            u_ref[:, cols(c, WC)] = t.astype(jnp.bfloat16)
        own_partial(s, 1, u_ref, wdown, wd_copy)

    lag = 5
    early = 4

    def forward(s, a, c):
        k = 2 * s + a
        part_copy(k, c).wait_recv()
        part[a, c] = (part[a, c].astype(jnp.float32) + in1[k, c].astype(jnp.float32)).astype(jnp.bfloat16)
        sum_copy(k, c).start()

    def leave(s, a, c):
        if a == 1:
            @pl.when(sends)
            def _():
                fwd_copy(s, c).start()
            out_copy(s, c).start()

    def finish(s, a, c):
        k = 2 * s + a
        bias = bo_ref if a == 0 else bd_ref
        sum_copy(k, c).wait_recv()
        resid = xbuf[s, c] if a == 0 else in1[2 * s, c]
        total = part[a, c].astype(jnp.float32) + in2[k, c].astype(jnp.float32)
        in1[k, c] = (resid.astype(jnp.float32) + total + bias[:, cols(c)].astype(jnp.float32)).astype(jnp.bfloat16)
        res_copy(k, c).start()
        leave(s, a, c)

    def reduce_inner(s, had, more):
        @pl.when(had)
        def _():
            @pl.loop(0, nc - 1)
            def _(i):
                forward(s - 1, 1, i)

                @pl.when(i >= lag)
                def _():
                    finish(s - 1, 1, i - lag)
            forward(s - 1, 1, nc - 1)
            finish(s - 1, 1, nc - 1 - lag)

        @pl.loop(0, early)
        def _(i):
            @pl.when(more)
            def _():
                forward(s, 0, i)

            @pl.when(had)
            def _():
                for j in range(2):
                    c = nc - lag + 2 * i + j

                    @pl.when(c < nc)
                    def _(c=c):
                        finish(s - 1, 1, c)

        @pl.when(more)
        def _():
            @pl.loop(early, nc + lag)
            def _(i):
                @pl.when(i < nc)
                def _():
                    forward(s, 0, i)

                @pl.when(i >= lag)
                def _():
                    finish(s, 0, i - lag)

    def reduce_outer(s, a):
        @pl.loop(0, nc)
        def _(c):
            part_copy(2 * s + a, c).wait_recv()
            leave(s, a, c)

    @pl.loop(0, micro_n + 1)
    def _(s):
        had = s > 0
        more = s < micro_n

        @pl.when(more)
        def _():
            p1(s)

        @pl.when(inner)
        def _():
            reduce_inner(s, had, more)

        @pl.when(outer)
        def _():
            @pl.when(had)
            def _():
                reduce_outer(s - 1, 1)

            @pl.when(more)
            def _():
                reduce_outer(s, 0)

        @pl.when(more)
        def _():
            p2(s)

    last = micro_n - 1
    for a in range(2):
        for c in range(nc):
            part_copy(2 * last + a, c).wait_send()

    @pl.when(inner)
    def _():
        @pl.loop(0, 2 * micro_n)
        def _(k):
            @pl.loop(0, nc)
            def _(c):
                res_copy(k, c).wait_send()

    @pl.loop(0, micro_n)
    def _(u):
        @pl.loop(0, nc)
        def _(c):
            @pl.when(sends)
            def _():
                fwd_copy(u, c).wait_send()
            out_copy(u, c).wait()


def solution(mesh):
    stages = mesh.shape['pp']
    in_specs = (P('dp'), P('dp'), P('pp'), P('pp'), P('pp', None, None, 'tp'), P('pp', None, 'tp', None), P('pp', 'tp', None), P('pp'), P('pp'), P('pp'), P('pp', None, 'tp'), P('pp', 'tp'), P('pp', 'tp', None), P('pp'))

    def per_device(x_in, seq_lens, ln1_gain, ln1_shift, w_qkv, b_qkv, w_out, b_out, ln2_gain, ln2_shift, w_up, b_up, w_down, b_down):
        micro_n, batch_n, seq_n, model_n = x_in.shape
        heads_loc, head_dim = b_qkv.shape[2], b_qkv.shape[3]
        width_loc = heads_loc * head_dim
        hid_loc = w_up.shape[2]
        nc, nw, nu = model_n // CH, model_n // WC, hid_loc // WC
        assert batch_n == 1 and mesh.shape['tp'] == 4 and seq_n == 128
        slopes = alibi_slopes(heads_loc * mesh.shape['tp'])
        bf = jnp.bfloat16
        vm = pl.BlockSpec(memory_space=pltpu.VMEM)
        sm = pl.BlockSpec(memory_space=pltpu.SMEM)
        hb = pl.BlockSpec(memory_space=pl.ANY)
        dma = pltpu.SemaphoreType.DMA
        body = functools.partial(kernel, stages, micro_n, seq_n, model_n, hid_loc, heads_loc, head_dim)
        out = pl.pallas_call(
            body,
            out_shape=jax.ShapeDtypeStruct((micro_n, seq_n, model_n), bf),
            in_specs=[sm, sm] + [hb] * 5 + [vm] * 8,
            out_specs=hb,
            scratch_shapes=[
                pltpu.VMEM((3, model_n, width_loc), bf),
                pltpu.VMEM((nw, width_loc, WC), bf),
                pltpu.VMEM((nu, model_n, WC), bf),
                pltpu.VMEM((nw, hid_loc, WC), bf),
                pltpu.VMEM((micro_n, nc, seq_n, CH), bf),
                pltpu.VMEM((2 * micro_n, nc, seq_n, CH), bf),
                pltpu.VMEM((2 * micro_n, nc, seq_n, CH), bf),
                pltpu.VMEM((2, nc, seq_n, CH), bf),
                pltpu.VMEM((seq_n, model_n), bf),
                pltpu.VMEM((seq_n, hid_loc), bf),
                pltpu.VMEM((3, seq_n, width_loc), bf),
                pltpu.VMEM((seq_n, width_loc), jnp.float32),
                pltpu.VMEM((seq_n, width_loc), bf),
                pltpu.VMEM((3, width_loc), jnp.float32),
                dma((3,)), dma((nw,)), dma((nu,)), dma((nw,)),
                dma((micro_n, nc)), dma((2 * micro_n, nc)), dma((2 * micro_n, nc)),
                dma((2 * micro_n, nc)), dma((2 * micro_n, nc)), dma((micro_n, nc)), dma((micro_n, nc)),
            ],
            compiler_params=pltpu.CompilerParams(
                collective_id=0, has_side_effects=True, vmem_limit_bytes=67043328),
            name='stages',
        )(
            seq_lens.reshape(micro_n), slopes,
            x_in.reshape(micro_n, seq_n, model_n),
            jnp.transpose(w_qkv[0], (1, 0, 2)), w_out[0], w_up[0], w_down[0],
            ln1_gain, ln1_shift, b_qkv, b_out, ln2_gain, ln2_shift, b_up, b_down,
        )
        return out.reshape(1, micro_n, batch_n, seq_n, model_n)

    return jax.shard_map(per_device, mesh=mesh, in_specs=in_specs, out_specs=P('pp', 'dp'), check_vma=False)
```
